1024 devices in a mesh: dom: 256 (over y, z, core), sub: 4 (over x).
Axes of the slice: x: 4, y: 8, z: 16, core: 2. Of those that a mesh axis runs over, the one named last changes fastest.
Arguments:
- dofs: float32 [9, 56, 16384], P(None, None, ('dom', 'sub')), may hold values from -6 to 6
- stiffness: float32 [3, 56, 56], replicated, may hold values from -0.75 to 0.75
- projection: float32 [4, 21, 56], replicated, may hold values from -0.75 to 0.75
- star: float32 [3, 9, 9, 16384], P(None, None, None, ('dom', 'sub')), may hold values from -1.25 to 1.25
- flux_minus: float32 [4, 9, 9, 16384], P(None, None, None, ('dom', 'sub')), may hold values from -1 to 1
- flux_plus: float32 [4, 9, 9, 16384], P(None, None, None, ('dom', 'sub')), may hold values from -1 to 1
- fault_flux: float32 [9, 9], replicated, may hold values from -2 to 2
- fault_faces: int32 [4, 16384], P(None, ('dom', 'sub')), may hold values 0 or 1
- levels: int32 [16384], P(('dom', 'sub')), may hold values from 0 to 1, as said below
- face_source: int32 [4, 16384], P(None, ('dom', 'sub')), may hold values from 0 to 111, as said below
- send_source: int32 [4096], P(('dom', 'sub')), may hold values from 0 to 63
Outputs:
- dofs_after: float32 [9, 56, 16384], P(None, None, ('dom', 'sub'))
The draws below stay inside these ranges and needn't reach their ends.
Inputs may be any that keep to these rules, and one draw needn't show every extreme that they name: `levels`: on every device at most 8 of its 16 elements have level 0, and some device has exactly 8. `face_source`: values below 64 name a face of the same device as face times 16 plus element; larger values name received exported faces as defined in the reference program.
All inputs are finite; a program needn't handle non-finite values. No bound on the sum of `fault_faces` on one device may be relied on, other than what follows from the above.
Results may differ from the reference program's by a relative error of at most 0.0001.
Values sent between devices are 32-bit elements; how exact they have to be, the bound alone decides.
A program may use at most 64 MiB of HBM per device.

```python
import math
import jax
import jax.numpy as jnp
from jax import lax

VARS = 9
MODES = 56
FACE_MODES = 21
ORDER = 6
E_DEV = 16
SEND = 4
FINE_MOST = 8
RECV = 48
ELEMS = 16384
N_DOM = 256
N_SUB = 4
DEVICES = 1024


def draw_levels(key, part):
    device_count = ELEMS // E_DEV
    key_count, key_busiest, key_ranks = jax.random.split(key, 3)
    counts = jax.random.randint(key_count, (device_count,), FINE_MOST // 4, FINE_MOST + 1)
    busiest = jax.random.randint(key_busiest, (), 0, device_count)
    counts = jnp.where(jnp.arange(device_count) == busiest, FINE_MOST, counts)
    ranks = jax.vmap(lambda single: jax.random.permutation(single, E_DEV))(jax.random.split(key_ranks, device_count))
    return jnp.where(ranks < counts[:, None], 0, 1).astype(jnp.int32).reshape(-1)


def draw_face_source(key, part):
    key_kind, key_local, key_remote = jax.random.split(key, 3)
    grid_shape = (4, ELEMS)
    choose_kind = jax.random.randint(key_kind, grid_shape, 0, 4)
    local_codes = jax.random.randint(key_local, grid_shape, 0, 4 * E_DEV)
    remote_codes = 4 * E_DEV + jax.random.randint(key_remote, grid_shape, 0, RECV)
    return jnp.where(choose_kind < 3, local_codes, remote_codes).astype(jnp.int32)


def touch_ends(result, key, least, high):
    extent = result.shape
    index_at = [jax.random.randint(jax.random.fold_in(key, axis), (), 0, extent[axis]) for axis in range(len(extent))]
    result = result.at[tuple(index_at)].set(least)
    longest = extent.index(max(extent))
    index_at[longest] = (index_at[longest] + 1) % extent[longest]
    return result.at[tuple(index_at)].set(high)


def block_scale(key, shape, cuts, least, largest):
    gain = 1.0
    for dim, blocks in cuts:
        heights = jax.random.uniform(jax.random.fold_in(jax.random.fold_in(key, 6), dim), (blocks,), jnp.float32, least / len(cuts), largest / len(cuts))
        gain = gain * jnp.repeat(jnp.exp(heights), shape[dim] // blocks).reshape((-1,) + (1,) * (len(shape) - 1 - dim))
    return gain


def bell_draw(stream_key, extent, width, most, cuts=(), kind=jnp.bfloat16):
    values = width * jax.random.normal(stream_key, extent, jnp.float32)
    if cuts:
        values = values * block_scale(stream_key, extent, cuts, -0.22, 0.18)
    return jnp.clip(values, -most, most).astype(kind)


def setup_inputs(seed: int = 0) -> dict:
    arg_keys = jax.random.split(jax.random.key(seed), 12)
    dofs = bell_draw(arg_keys[0], (VARS, MODES, ELEMS), 1.0, 6.0, ((2, 1024),), jnp.float32)
    stiffness = bell_draw(arg_keys[1], (3, MODES, MODES), MODES ** -0.5, 0.75, (), jnp.float32)
    projection = bell_draw(arg_keys[2], (4, FACE_MODES, MODES), MODES ** -0.5, 0.75, (), jnp.float32)
    star = bell_draw(arg_keys[3], (3, VARS, VARS, ELEMS), 27 ** -0.5, 1.25, ((3, 1024),), jnp.float32)
    flux_minus = bell_draw(arg_keys[4], (4, VARS, VARS, ELEMS), 36 ** -0.5, 1.0, ((3, 1024),), jnp.float32)
    flux_plus = bell_draw(arg_keys[5], (4, VARS, VARS, ELEMS), 36 ** -0.5, 1.0, ((3, 1024),), jnp.float32)
    fault_flux = bell_draw(arg_keys[6], (VARS, VARS), 9 ** -0.5, 2.0, (), jnp.float32)
    fault_faces = touch_ends((jax.random.randint(arg_keys[7], (4, ELEMS), 0, 8) < 1).astype(jnp.int32), jax.random.fold_in(arg_keys[7], 1), 0, 1)
    levels = draw_levels(jax.random.fold_in(arg_keys[11], 71), 0)
    face_source = draw_face_source(jax.random.fold_in(arg_keys[11], 71), 0)
    send_source = touch_ends(jax.random.randint(arg_keys[10], (SEND * DEVICES,), 0, 4 * E_DEV), jax.random.fold_in(arg_keys[10], 1), 0, (4 * E_DEV) - 1).astype(jnp.int32)
    return dict(dofs=dofs, stiffness=stiffness, projection=projection, star=star, flux_minus=flux_minus, flux_plus=flux_plus, fault_flux=fault_flux, fault_faces=fault_faces, levels=levels, face_source=face_source, send_source=send_source)


fine_step = 0.75
exact_reference = lax.Precision.HIGHEST


def taylor_weights(start_time, stop_time, term_count):
    return [(stop_time ** (term + 1) - start_time ** (term + 1)) / math.factorial(term + 1) for term in range(term_count)]


def derivatives(state_now, stiffness, star_contribution):
    taylor_series = [state_now]
    for repeat in range(ORDER - 1):
        time_slopes = jnp.einsum("dmn,wne->dwme", stiffness, taylor_series[-1], precision=exact_reference)
        taylor_series.append(jnp.einsum("usij,uifj->sfj", star_contribution, time_slopes, precision=exact_reference))
    return jnp.stack(taylor_series)


def integrate(taylor_series, start_time, stop_time):
    quadrature_weights = jnp.array(taylor_weights(start_time, stop_time, taylor_series.shape[0]), jnp.float32)
    return jnp.einsum("h,hlui->lui", quadrature_weights, taylor_series, precision=exact_reference)


def face_values(field_state, projection):
    return jnp.einsum("bly,qyp->qlbp", projection, field_state, precision=exact_reference)


def advance(state_now, own_part, own_faces, beside, stiffness, projection, star_contribution, minus_part, coupling_part):
    incoming_flux = jnp.einsum("dvwe,wne->dvne", star_contribution, own_part, precision=exact_reference)
    volume_term = jnp.einsum("utx,uytz->yxz", stiffness, incoming_flux, precision=exact_reference)
    flux_terms = jnp.einsum("fvwe,wjfe->vjfe", minus_part, own_faces, precision=exact_reference)
    flux_terms = flux_terms + jnp.einsum("fvwe,wjfe->vjfe", coupling_part, beside, precision=exact_reference)
    surface_term = jnp.einsum("alz,qlad->qzd", projection, flux_terms, precision=exact_reference)
    return state_now + volume_term - surface_term


def to_blocks(array):
    split = array.reshape(array.shape[:-1] + (ELEMS // E_DEV, E_DEV))
    return jnp.moveaxis(split, -2, 0)


def from_blocks(array):
    joined = jnp.moveaxis(array, 0, -2)
    return joined.reshape(joined.shape[:-2] + (ELEMS,))


def reference(dofs, stiffness, projection, star, flux_minus, flux_plus, fault_flux, fault_faces, levels, face_source, send_source):
    device_count = ELEMS // E_DEV
    coupling = jnp.where(fault_faces[:, None, None, :] == 1, fault_flux[None, :, :, None], flux_plus)
    element_ids = jnp.arange(ELEMS, dtype=jnp.int32)
    device_ids = (element_ids // E_DEV)[None, :]
    local_column = device_ids * (4 * E_DEV) + face_source
    offset = face_source - 4 * E_DEV
    side_index = offset // (N_SUB * SEND)
    sub_index = (offset // SEND) % N_SUB
    slot_index = offset % SEND
    source_device = ((device_ids // N_SUB + side_index - 1) % N_DOM) * N_SUB + sub_index
    send_position = jnp.clip(source_device * SEND + slot_index, 0, device_count * SEND - 1).astype(jnp.int32)
    remote_column = source_device * (4 * E_DEV) + send_source[send_position]
    column = jnp.where(face_source < 4 * E_DEV, local_column, remote_column).astype(jnp.int32)
    column_order = to_blocks(column).reshape(-1)

    def beside_values(face_blocks):
        source_table = jnp.moveaxis(face_blocks, 0, 2).reshape(VARS * FACE_MODES, -1)
        picked = jnp.take(source_table, column_order, axis=1)
        return jnp.moveaxis(picked.reshape(VARS, FACE_MODES, device_count, 4, E_DEV), 2, 0)

    block_dofs = to_blocks(dofs)
    block_star = to_blocks(star)
    block_minus = to_blocks(flux_minus)
    block_coupling = to_blocks(coupling)
    block_fine = to_blocks(levels == 0)

    def phase_one(items):
        state_now, star_contribution = items
        taylor_series = derivatives(state_now, stiffness, star_contribution)
        first_half = integrate(taylor_series, 0.0, fine_step)
        second_half = integrate(taylor_series, fine_step, 2.0 * fine_step)
        return first_half, second_half, face_values(first_half, projection)

    first_b, second_b, first_faces_b = lax.map(phase_one, (block_dofs, block_star))
    beside_first_b = beside_values(first_faces_b)

    def phase_two(items):
        state_now, star_contribution, minus_part, coupling_part, is_fine, first_half, second_half, first_faces, beside_first = items
        updated = advance(state_now, first_half, first_faces, beside_first, stiffness, projection, star_contribution, minus_part, coupling_part)
        state_one = jnp.where(is_fine, updated, state_now)
        fine_integral = integrate(derivatives(state_one, stiffness, star_contribution), 0.0, fine_step)
        carried = jnp.where(is_fine, fine_integral, second_half)
        return state_one, carried, face_values(carried, projection)

    state_one_b, carried_b, carried_faces_b = lax.map(phase_two, (block_dofs, block_star, block_minus, block_coupling, block_fine, first_b, second_b, first_faces_b, beside_first_b))
    beside_carried_b = beside_values(carried_faces_b)

    def phase_three(items):
        state_now, star_contribution, minus_part, coupling_part, is_fine, first_half, second_half, beside_first, state_one, carried, carried_faces, beside_carried = items
        fine_new = advance(state_one, carried, carried_faces, beside_carried, stiffness, projection, star_contribution, minus_part, coupling_part)
        whole_step = first_half + second_half
        coarse_new = advance(state_now, whole_step, face_values(whole_step, projection), beside_first + beside_carried, stiffness, projection, star_contribution, minus_part, coupling_part)
        return jnp.where(is_fine, fine_new, coarse_new)

    result_b = lax.map(phase_three, (block_dofs, block_star, block_minus, block_coupling, block_fine, first_b, second_b, beside_first_b, state_one_b, carried_b, carried_faces_b, beside_carried_b))
    return from_blocks(result_b)
```

```python
import functools
import math

import jax
import jax.numpy as jnp
from jax import lax
from jax.experimental import pallas as pl
from jax.experimental.pallas import tpu as pltpu
from jax.sharding import PartitionSpec as P

ORDER = 6
TAU = 0.75
V = 9
M = 56
J = 21
E = 16
SLOTS = 12
MESH = pl.DeviceIdType.MESH
F32 = jnp.float32
BF16 = jnp.bfloat16


def taylor_weights(start_time, stop_time):
    return [
        (stop_time ** (k + 1) - start_time ** (k + 1)) / math.factorial(k + 1)
        for k in range(ORDER)
    ]


FIRST = taylor_weights(0.0, TAU)
SECOND = taylor_weights(TAU, 2.0 * TAU)


def split(x):
    hi = x.astype(BF16)
    return hi, (x - hi.astype(F32)).astype(BF16)


def lhs3(x):
    hi, lo = split(x)
    return jnp.concatenate([hi, lo, hi], axis=1)


def rhs3(x):
    hi, lo = split(x)
    return jnp.concatenate([hi, hi, lo], axis=0)


def stack2(x):
    hi, lo = split(x)
    return jnp.concatenate([hi, lo], axis=0)


def dot(a, b):
    return jnp.dot(a, b, preferred_element_type=F32)


def lanes(shape=(8, 128)):
    return lax.broadcasted_iota(jnp.int32, shape, 1)


def rows(shape=(8, 128)):
    return lax.broadcasted_iota(jnp.int32, shape, 0)


def roll(x, shift):
    return pltpu.roll(x, shift % 128, 1)


def swap_blocks(a):
    lane = lanes()
    low = lane < 64
    even = (lane // 32) % 2 == 0
    p0 = jnp.where(low, a[0], roll(a[2], 64))
    p2 = jnp.where(low, roll(a[0], 64), a[2])
    p1 = jnp.where(low, a[1], roll(a[3], 64))
    p3 = jnp.where(low, roll(a[1], 64), a[3])
    return [
        jnp.where(even, p0, roll(p1, 32)),
        jnp.where(even, roll(p0, -32), p1),
        jnp.where(even, p2, roll(p3, 32)),
        jnp.where(even, roll(p2, -32), p3),
    ]


def to_table(faces):
    lane = lanes()
    ends = (lane >= J) & (lane < 32)
    more = (lane >= 32 + J) & (lane < 42 + J)
    first, second = [], []
    for half in range(2):
        part = [faces[8 * w : 8 * w + 8, 128 * half : 128 * half + 128] for w in range(V)]
        one = swap_blocks(part[0:4])
        two = swap_blocks(part[4:8])
        for b in range(4):
            kept = jnp.where(ends, roll(part[8], J - 32 * b), one[b])
            first.append(jnp.where(more, roll(part[8], 42 - 32 * b), kept))
            second.append(two[b])
    return jnp.concatenate(first, axis=0), jnp.concatenate(second, axis=0)


def from_table(first, second):
    lane = lanes()
    halves = []
    for half in range(2):
        one = [first[32 * half + 8 * b : 32 * half + 8 * b + 8] for b in range(4)]
        two = [second[32 * half + 8 * b : 32 * half + 8 * b + 8] for b in range(4)]
        last = jnp.zeros((8, 128), F32)
        for b in range(4):
            inside = lane - 32 * b
            last = jnp.where((inside >= 0) & (inside < 11), roll(one[b], 32 * b - J), last)
            last = jnp.where((inside >= 11) & (inside < J), roll(one[b], 32 * b - 42), last)
        halves.append(swap_blocks(one) + swap_blocks(two) + [last])
    return [jnp.concatenate([halves[0][w], halves[1][w]], axis=1) for w in range(V)]


def kernel(
    n_dom,
    n_sub,
    levels_ref,
    source_ref,
    send_ref,
    fault_flux_ref,
    fault_faces_ref,
    dofs_hbm,
    stiff_hbm,
    proj_hbm,
    star_hbm,
    minus_hbm,
    plus_hbm,
    out_ref,
    dofs_ref,
    stiff_ref,
    proj_ref,
    star_ref,
    minus_ref,
    plus_ref,
    block_ref,
    pt_ref,
    x_ref,
    row_ref,
    wd_ref,
    wv_ref,
    pw_ref,
    pt3_ref,
    cs_ref,
    cm_ref,
    cc_ref,
    flux_ref,
    msg_ref,
    recv_ref,
    in_sem,
    send_sem,
    recv_sem,
):
    dom = lax.axis_index("dom")
    sub = lax.axis_index("sub")
    peers = []
    for delta in (-1, 1, 0):
        for turn in (2, 1, 3, 0):
            if delta == 0 and turn == 0:
                continue
            peers.append((delta, lax.rem(dom + delta + n_dom, n_dom), lax.rem(sub + turn, n_sub)))

    barrier = pltpu.get_barrier_semaphore()
    for _, to_dom, to_sub in peers:
        pl.semaphore_signal(barrier, inc=1, device_id=(to_dom, to_sub), device_id_type=MESH)

    loads = [
        pltpu.make_async_copy(src, dst, in_sem.at[i])
        for i, (src, dst) in enumerate(
            (
                (stiff_hbm, stiff_ref),
                (star_hbm, star_ref),
                (dofs_hbm, dofs_ref),
                (proj_hbm, proj_ref),
                (minus_hbm, minus_ref),
                (plus_hbm, plus_ref),
            )
        )
    ]
    for load in loads:
        load.start()

    block_ref[...] = jnp.zeros(block_ref.shape, F32)
    pt_ref[...] = jnp.zeros(pt_ref.shape, F32)
    x_ref[...] = jnp.zeros(x_ref.shape, F32)
    row_ref[...] = jnp.zeros(row_ref.shape, F32)

    loads[0].wait()
    for d in range(3):
        block_ref[d, 0:M, 0:M] = stiff_ref[d]
        block_ref[d, 64 : 64 + M, 64 : 64 + M] = stiff_ref[d]
    for d in range(3):
        block = block_ref[d]
        wd_ref[:, 128 * d : 128 * d + 128] = rhs3(block.T)
        wv_ref[:, 128 * d : 128 * d + 128] = rhs3(block)

    def spread(make_row, groups, part_width, fill, coef_ref):
        width = 128 * coef_ref.shape[3] // 128
        k = lax.broadcasted_iota(jnp.int32, (128, width), 0) % 64
        lane = lax.broadcasted_iota(jnp.int32, (128, width), 1)
        group = lane // (2 * part_width)
        half = (lane // part_width) % 2
        hit = (k // E == group) & ((k % E) // 8 == half) & (lane % part_width < fill)
        repeat = hit.astype(F32).astype(BF16)
        keep = (lanes() % 8 == rows()).astype(F32)
        for v in range(V):
            row = make_row(v)
            high = row.astype(BF16).astype(F32)
            row_ref[v, 0:V, 0 : groups * E] = high
            row_ref[v, 0:V, 64 : 64 + groups * E] = row - high
        for v in range(V):
            left = jnp.concatenate(
                [jnp.broadcast_to(row_ref[v, w : w + 1, :], (8, 128)) * keep for w in range(V)],
                axis=0,
            ).astype(BF16)
            coef_ref[v] = dot(left, repeat).reshape(V, 8, width)

    loads[1].wait()
    spread(
        lambda v: jnp.concatenate([star_ref[v, :, d, :] for d in range(3)], axis=1),
        3,
        64,
        M,
        cs_ref,
    )

    loads[2].wait()
    for v in range(V):
        x_ref[8 * v : 8 * v + 8, 0:M] = dofs_ref[v, 0:8, :]
        x_ref[8 * v : 8 * v + 8, 64 : 64 + M] = dofs_ref[v, 8:16, :]

    def contract(coef_ref, field, v):
        return (coef_ref[v] * field).sum(axis=0)

    def with_star(weights_ref, left):
        field = dot(left, weights_ref[...]).reshape(V, 8, 384)
        result = []
        for v in range(V):
            total = contract(cs_ref, field, v)
            result.append(total[:, 0:128] + total[:, 128:256] + total[:, 256:384])
        return jnp.concatenate(result, axis=0)

    def series(start, want_second):
        current = start
        first = FIRST[0] * current
        second = SECOND[0] * current if want_second else None
        for k in range(1, ORDER):
            current = with_star(wd_ref, lhs3(current))
            first = first + FIRST[k] * current
            if want_second:
                second = second + SECOND[k] * current
        return first, second

    dofs = x_ref[...]
    first_half, second_half = series(dofs, True)

    loads[3].wait()
    for f in range(4):
        for half in range(2):
            at = 64 * f + 32 * half
            pt_ref[at : at + J, 64 * half : 64 * half + M] = proj_ref[:, f, :]
    pt = pt_ref[...]
    pw_ref[...] = rhs3(pt.T)
    pt3_ref[...] = rhs3(pt)

    row = rows((8, 256))
    lane = lanes((8, 256))
    wanted = jnp.full((8, 256), -1, jnp.int32)
    for s in range(4):
        wanted = jnp.where(row % 4 == s, send_ref[s], wanted)
    pick_send = ((lane % 64 == wanted) & (lane // 128 == row // 4)).astype(F32).astype(BF16)

    local_rows, remote_rows = [], []
    row = rows()
    lane = lanes()
    lane2 = lanes((8, 192)) % 96
    for f in range(4):
        for half in range(2):
            wanted = jnp.full((8, 128), -1, jnp.int32)
            for i in range(8):
                wanted = jnp.where(row == i, source_ref[f, 8 * half + i], wanted)
            local_rows.append((lane % 64 == wanted).astype(F32))
            far = wanted - 64
            code = jnp.where(far >= 0, (far // 4) * 8 + far % 4, -8)
            code = jnp.concatenate([code, code[:, 0:64]], axis=1)
            remote_rows.append((code, lane2))
    pick_local = jnp.concatenate(local_rows, axis=0).astype(BF16)
    pick_remote = jnp.concatenate(
        [(at == code + 4 * q).astype(F32) for q in range(2) for code, at in remote_rows], axis=0
    ).astype(BF16)

    fine = jnp.zeros((8, 128), jnp.int32)
    for e in range(E):
        here = (row == e % 8) & (lane // 64 == e // 8)
        fine = jnp.where(here & (levels_ref[e] == 0), 1, fine)
    fine = jnp.concatenate([fine] * V, axis=0) == 1

    def start_exchange(turn, table):
        stacked = jnp.concatenate([stack2(table[0]), stack2(table[1])], axis=0)
        message = dot(pick_send, stacked)
        msg_ref[turn] = message
        recv_ref[turn, 4 + sub] = message
        copies = []
        for delta, to_dom, to_sub in peers:
            copies.append(
                pltpu.make_async_remote_copy(
                    src_ref=msg_ref.at[turn],
                    dst_ref=recv_ref.at[turn, 4 * (1 - delta) + sub],
                    send_sem=send_sem.at[turn, len(copies)],
                    recv_sem=recv_sem.at[turn, 4 * (1 - delta) + sub],
                    device_id=(to_dom, to_sub),
                    device_id_type=MESH,
                )
            )
        return copies

    def finish_exchange(turn, copies):
        for delta in (-1, 0, 1):
            for shift in range(4):
                if delta == 0 and shift == 0:
                    continue
                slot = 4 * (1 - delta) + lax.rem(sub + shift, n_sub)
                pltpu.make_async_remote_copy(
                    src_ref=msg_ref.at[turn],
                    dst_ref=recv_ref.at[turn, slot],
                    send_sem=send_sem.at[turn, 0],
                    recv_sem=recv_sem.at[turn, slot],
                    device_id=(dom, lax.rem(sub + 1, n_sub)),
                    device_id_type=MESH,
                ).wait_recv()

    def local_part(table):
        return dot(pick_local, jnp.concatenate([stack2(table[0]), stack2(table[1])], axis=1))

    def beside_faces(turn, near):
        far = dot(pick_remote, stack2(recv_ref[turn].reshape(8 * SLOTS, 128)))
        faces = from_table(near[:, 0:128] + far[0:64], near[:, 128:256] + far[64:128])
        return jnp.concatenate(faces, axis=0).reshape(V, 8, 256)

    left = lhs3(first_half)
    faces = dot(left, pw_ref[...])
    table = to_table(faces)
    copies = start_exchange(0, table)
    pl.semaphore_wait(barrier, len(peers))
    for copy in copies:
        copy.start()
    sent = list(copies)

    loads[4].wait()
    spread(
        lambda v: jnp.concatenate([minus_ref[v, :, f, :] for f in range(4)], axis=1),
        4,
        32,
        J,
        cm_ref,
    )
    loads[5].wait()
    on_fault = jnp.concatenate([fault_faces_ref[f : f + 1, :] for f in range(4)], axis=1) == 1

    def coupling_row(v):
        plus = jnp.concatenate([plus_ref[v, :, f, :] for f in range(4)], axis=1)
        w_at = rows((V, 4 * E))
        friction = jnp.zeros((V, 4 * E), F32)
        for w in range(V):
            friction = jnp.where(w_at == w, fault_flux_ref[v, w], friction)
        return jnp.where(jnp.broadcast_to(on_fault, (V, 4 * E)), friction, plus)

    spread(coupling_row, 4, 32, J, cc_ref)

    def own_side(left, faces):
        volume = with_star(wv_ref, left)
        field = faces.reshape(V, 8, 256)
        for v in range(V):
            flux_ref[8 * v : 8 * v + 8, :] = contract(cm_ref, field, v)
        return volume

    def far_side(base, turn, near):
        field = beside_faces(turn, near)
        total = jnp.concatenate([contract(cc_ref, field, v) for v in range(V)], axis=0)
        return base - dot(lhs3(total + flux_ref[...]), pt3_ref[...])

    near = local_part(table)
    base = dofs + own_side(left, faces)
    finish_exchange(0, copies)
    moved = far_side(base, 0, near)

    again, _ = series(moved, False)
    carried = jnp.where(fine, again, second_half)
    left = lhs3(carried)
    faces = dot(left, pw_ref[...])
    table = to_table(faces)
    copies = start_exchange(1, table)
    for copy in copies:
        copy.start()
    sent += copies
    near = local_part(table)
    base = moved + own_side(left, faces)
    finish_exchange(1, copies)
    after = far_side(base, 1, near)
    for v in range(V):
        out_ref[v, 0:8, :] = after[8 * v : 8 * v + 8, 0:M]
        out_ref[v, 8:16, :] = after[8 * v : 8 * v + 8, 64 : 64 + M]
    for copy in sent:
        copy.wait_send()


def per_device(
    n_dom,
    n_sub,
    dofs,
    stiffness,
    projection,
    star,
    flux_minus,
    flux_plus,
    fault_flux,
    fault_faces,
    levels,
    face_source,
    send_source,
):
    smem = pl.BlockSpec(memory_space=pltpu.SMEM)
    vmem = pl.BlockSpec(memory_space=pltpu.VMEM)
    hbm = pl.BlockSpec(memory_space=pl.ANY)
    result = pl.pallas_call(
        functools.partial(kernel, n_dom, n_sub),
        out_shape=jax.ShapeDtypeStruct((V, E, M), F32),
        in_specs=[smem] * 4 + [vmem] + [hbm] * 6,
        out_specs=vmem,
        scratch_shapes=[
            pltpu.VMEM((V, E, M), F32),
            pltpu.VMEM((3, M, M), F32),
            pltpu.VMEM((J, 4, M), F32),
            pltpu.VMEM((V, V, 3, E), F32),
            pltpu.VMEM((V, V, 4, E), F32),
            pltpu.VMEM((V, V, 4, E), F32),
            pltpu.VMEM((3, 128, 128), F32),
            pltpu.VMEM((256, 128), F32),
            pltpu.VMEM((72, 128), F32),
            pltpu.VMEM((V, 16, 128), F32),
            pltpu.VMEM((384, 384), BF16),
            pltpu.VMEM((384, 384), BF16),
            pltpu.VMEM((384, 256), BF16),
            pltpu.VMEM((768, 128), BF16),
            pltpu.VMEM((V, V, 8, 384), F32),
            pltpu.VMEM((V, V, 8, 256), F32),
            pltpu.VMEM((V, V, 8, 256), F32),
            pltpu.VMEM((72, 256), F32),
            pltpu.VMEM((2, 8, 128), F32),
            pltpu.VMEM((2, SLOTS, 8, 128), F32),
            pltpu.SemaphoreType.DMA((6,)),
            pltpu.SemaphoreType.DMA((2, SLOTS)),
            pltpu.SemaphoreType.DMA((2, SLOTS)),
        ],
        compiler_params=pltpu.CompilerParams(collective_id=0, has_side_effects=True),
    )(
        levels,
        face_source,
        send_source,
        fault_flux,
        fault_faces,
        jnp.transpose(dofs, (0, 2, 1)),
        stiffness,
        jnp.transpose(projection, (1, 0, 2)),
        jnp.transpose(star, (1, 2, 0, 3)),
        jnp.transpose(flux_minus, (1, 2, 0, 3)),
        jnp.transpose(flux_plus, (1, 2, 0, 3)),
    )
    return jnp.transpose(result, (0, 2, 1))


def solution(mesh):
    return jax.shard_map(
        functools.partial(per_device, mesh.shape["dom"], mesh.shape["sub"]),
        mesh=mesh,
        in_specs=(
            P(None, None, ("dom", "sub")),
            P(),
            P(),
            P(None, None, None, ("dom", "sub")),
            P(None, None, None, ("dom", "sub")),
            P(None, None, None, ("dom", "sub")),
            P(),
            P(None, ("dom", "sub")),
            P(("dom", "sub")),
            P(None, ("dom", "sub")),
            P(("dom", "sub")),
        ),
        out_specs=P(None, None, ("dom", "sub")),
        check_vma=False,
    )
```

```python
import functools
import math

import jax
import jax.numpy as jnp
from jax import lax
from jax.experimental import pallas as pl
from jax.experimental.pallas import tpu as pltpu
from jax.sharding import PartitionSpec as P

ORDER = 6
TAU = 0.75
V = 9
M = 56
J = 21
E = 16
SLOTS = 12
VMEM_LIMIT = 24 * 2**20
MESH = pl.DeviceIdType.MESH
F32 = jnp.float32
BF16 = jnp.bfloat16


def taylor_weights(start_time, stop_time):
    return [
        (stop_time ** (k + 1) - start_time ** (k + 1)) / math.factorial(k + 1)
        for k in range(ORDER)
    ]


FIRST = taylor_weights(0.0, TAU)
SECOND = taylor_weights(TAU, 2.0 * TAU)


def split(x):
    hi = x.astype(BF16)
    return hi, (x - hi.astype(F32)).astype(BF16)


def lhs3(x):
    hi, lo = split(x)
    return jnp.concatenate([hi, lo, hi], axis=1)


def rhs3(x):
    hi, lo = split(x)
    return jnp.concatenate([hi, hi, lo], axis=0)


def stack2(x):
    hi, lo = split(x)
    return jnp.concatenate([hi, lo], axis=0)


def dot(a, b):
    return jnp.dot(a, b, preferred_element_type=F32)


def lanes(shape=(8, 128)):
    return lax.broadcasted_iota(jnp.int32, shape, 1)


def rows(shape=(8, 128)):
    return lax.broadcasted_iota(jnp.int32, shape, 0)


def roll(x, shift):
    return pltpu.roll(x, shift % 128, 1)


def swap_blocks(a):
    lane = lanes()
    low = lane < 64
    even = (lane // 32) % 2 == 0
    p0 = jnp.where(low, a[0], roll(a[2], 64))
    p2 = jnp.where(low, roll(a[0], 64), a[2])
    p1 = jnp.where(low, a[1], roll(a[3], 64))
    p3 = jnp.where(low, roll(a[1], 64), a[3])
    return [
        jnp.where(even, p0, roll(p1, 32)),
        jnp.where(even, roll(p0, -32), p1),
        jnp.where(even, p2, roll(p3, 32)),
        jnp.where(even, roll(p2, -32), p3),
    ]


def to_table(faces):
    lane = lanes()
    ends = (lane >= J) & (lane < 32)
    more = (lane >= 32 + J) & (lane < 42 + J)
    first, second = [], []
    for half in range(2):
        part = [faces[8 * w : 8 * w + 8, 128 * half : 128 * half + 128] for w in range(V)]
        one = swap_blocks(part[0:4])
        two = swap_blocks(part[4:8])
        for b in range(4):
            kept = jnp.where(ends, roll(part[8], J - 32 * b), one[b])
            first.append(jnp.where(more, roll(part[8], 42 - 32 * b), kept))
            second.append(two[b])
    return jnp.concatenate(first, axis=0), jnp.concatenate(second, axis=0)


def from_table(first, second):
    lane = lanes()
    halves = []
    for half in range(2):
        one = [first[32 * half + 8 * b : 32 * half + 8 * b + 8] for b in range(4)]
        two = [second[32 * half + 8 * b : 32 * half + 8 * b + 8] for b in range(4)]
        last = jnp.zeros((8, 128), F32)
        for b in range(4):
            inside = lane - 32 * b
            last = jnp.where((inside >= 0) & (inside < 11), roll(one[b], 32 * b - J), last)
            last = jnp.where((inside >= 11) & (inside < J), roll(one[b], 32 * b - 42), last)
        halves.append(swap_blocks(one) + swap_blocks(two) + [last])
    return [jnp.concatenate([halves[0][w], halves[1][w]], axis=1) for w in range(V)]


def kernel(
    n_dom,
    n_sub,
    levels_hbm,
    source_hbm,
    send_hbm,
    fault_flux_hbm,
    fault_faces_hbm,
    dofs_hbm,
    stiff_hbm,
    proj_hbm,
    star_hbm,
    minus_hbm,
    plus_hbm,
    out_ref,
    levels_ref,
    source_ref,
    send_ref,
    fault_flux_ref,
    fault_faces_ref,
    dofs_ref,
    stiff_ref,
    proj_ref,
    star_ref,
    minus_ref,
    plus_ref,
    block_ref,
    pt_ref,
    x_ref,
    row_ref,
    wd_ref,
    wv_ref,
    pw_ref,
    pt3_ref,
    cs_ref,
    cm_ref,
    cc_ref,
    flux_ref,
    msg_ref,
    recv_ref,
    in_sem,
    send_sem,
    recv_sem,
):
    dom = lax.axis_index("dom")
    sub = lax.axis_index("sub")
    peers = []
    for delta in (-1, 1, 0):
        for turn in (2, 1, 3, 0):
            if delta == 0 and turn == 0:
                continue
            peers.append((delta, lax.rem(dom + delta + n_dom, n_dom), lax.rem(sub + turn, n_sub)))

    barrier = pltpu.get_barrier_semaphore()
    for _, to_dom, to_sub in peers:
        pl.semaphore_signal(barrier, inc=1, device_id=(to_dom, to_sub), device_id_type=MESH)

    loads = [
        pltpu.make_async_copy(src, dst, in_sem.at[i])
        for i, (src, dst) in enumerate(
            (
                (stiff_hbm, stiff_ref),
                (star_hbm, star_ref),
                (dofs_hbm, dofs_ref),
                (proj_hbm, proj_ref),
                (minus_hbm, minus_ref),
                (plus_hbm, plus_ref),
                (levels_hbm, levels_ref),
                (source_hbm, source_ref),
                (send_hbm, send_ref),
                (fault_flux_hbm, fault_flux_ref),
                (fault_faces_hbm, fault_faces_ref),
            )
        )
    ]
    for load in loads:
        load.start()

    block_ref[...] = jnp.zeros(block_ref.shape, F32)
    pt_ref[...] = jnp.zeros(pt_ref.shape, F32)
    x_ref[...] = jnp.zeros(x_ref.shape, F32)
    row_ref[...] = jnp.zeros(row_ref.shape, F32)

    loads[0].wait()
    for d in range(3):
        block_ref[d, 0:M, 0:M] = stiff_ref[d]
        block_ref[d, 64 : 64 + M, 64 : 64 + M] = stiff_ref[d]
    for d in range(3):
        block = block_ref[d]
        wd_ref[:, 128 * d : 128 * d + 128] = rhs3(block.T)
        wv_ref[:, 128 * d : 128 * d + 128] = rhs3(block)

    def spread(make_row, groups, part_width, fill, coef_ref):
        width = 128 * coef_ref.shape[3] // 128
        k = lax.broadcasted_iota(jnp.int32, (128, width), 0) % 64
        lane = lax.broadcasted_iota(jnp.int32, (128, width), 1)
        group = lane // (2 * part_width)
        half = (lane // part_width) % 2
        hit = (k // E == group) & ((k % E) // 8 == half) & (lane % part_width < fill)
        repeat = hit.astype(F32).astype(BF16)
        keep = (lanes() % 8 == rows()).astype(F32)
        for v in range(V):
            row = make_row(v)
            high = row.astype(BF16).astype(F32)
            row_ref[v, 0:V, 0 : groups * E] = high
            row_ref[v, 0:V, 64 : 64 + groups * E] = row - high
        for v in range(V):
            left = jnp.concatenate(
                [jnp.broadcast_to(row_ref[v, w : w + 1, :], (8, 128)) * keep for w in range(V)],
                axis=0,
            ).astype(BF16)
            coef_ref[v] = dot(left, repeat).reshape(V, 8, width)

    loads[1].wait()
    spread(
        lambda v: jnp.concatenate([star_ref[v, :, d, :] for d in range(3)], axis=1),
        3,
        64,
        M,
        cs_ref,
    )

    loads[2].wait()
    for v in range(V):
        x_ref[8 * v : 8 * v + 8, 0:M] = dofs_ref[v, 0:8, :]
        x_ref[8 * v : 8 * v + 8, 64 : 64 + M] = dofs_ref[v, 8:16, :]

    def contract(coef_ref, field, v):
        return (coef_ref[v] * field).sum(axis=0)

    def with_star(weights_ref, left):
        field = dot(left, weights_ref[...]).reshape(V, 8, 384)
        result = []
        for v in range(V):
            total = contract(cs_ref, field, v)
            result.append(total[:, 0:128] + total[:, 128:256] + total[:, 256:384])
        return jnp.concatenate(result, axis=0)

    def series(start, want_second):
        current = start
        first = FIRST[0] * current
        second = SECOND[0] * current if want_second else None
        for k in range(1, ORDER):
            current = with_star(wd_ref, lhs3(current))
            first = first + FIRST[k] * current
            if want_second:
                second = second + SECOND[k] * current
        return first, second

    dofs = x_ref[...]
    first_half, second_half = series(dofs, True)

    loads[3].wait()
    for f in range(4):
        for half in range(2):
            at = 64 * f + 32 * half
            pt_ref[at : at + J, 64 * half : 64 * half + M] = proj_ref[:, f, :]
    pt = pt_ref[...]
    pw_ref[...] = rhs3(pt.T)
    pt3_ref[...] = rhs3(pt)

    for i in (6, 7, 8):
        loads[i].wait()
    row = rows((8, 256))
    lane = lanes((8, 256))
    wanted = jnp.full((8, 256), -1, jnp.int32)
    for s in range(4):
        wanted = jnp.where(row % 4 == s, send_ref[s], wanted)
    pick_send = ((lane % 64 == wanted) & (lane // 128 == row // 4)).astype(F32).astype(BF16)

    local_rows, remote_rows = [], []
    row = rows()
    lane = lanes()
    lane2 = lanes((8, 192)) % 96
    for f in range(4):
        for half in range(2):
            wanted = jnp.full((8, 128), -1, jnp.int32)
            for i in range(8):
                wanted = jnp.where(row == i, source_ref[f, 8 * half + i], wanted)
            local_rows.append((lane % 64 == wanted).astype(F32))
            far = wanted - 64
            code = jnp.where(far >= 0, (far // 4) * 8 + far % 4, -8)
            code = jnp.concatenate([code, code[:, 0:64]], axis=1)
            remote_rows.append((code, lane2))
    pick_local = jnp.concatenate(local_rows, axis=0).astype(BF16)
    pick_remote = jnp.concatenate(
        [(at == code + 4 * q).astype(F32) for q in range(2) for code, at in remote_rows], axis=0
    ).astype(BF16)

    fine = jnp.zeros((8, 128), jnp.int32)
    for e in range(E):
        here = (row == e % 8) & (lane // 64 == e // 8)
        fine = jnp.where(here & (levels_ref[e] == 0), 1, fine)
    fine = jnp.concatenate([fine] * V, axis=0) == 1

    def start_exchange(turn, table):
        stacked = jnp.concatenate([stack2(table[0]), stack2(table[1])], axis=0)
        message = dot(pick_send, stacked)
        msg_ref[turn] = message
        recv_ref[turn, 4 + sub] = message
        copies = []
        for delta, to_dom, to_sub in peers:
            copies.append(
                pltpu.make_async_remote_copy(
                    src_ref=msg_ref.at[turn],
                    dst_ref=recv_ref.at[turn, 4 * (1 - delta) + sub],
                    send_sem=send_sem.at[turn, len(copies)],
                    recv_sem=recv_sem.at[turn, 4 * (1 - delta) + sub],
                    device_id=(to_dom, to_sub),
                    device_id_type=MESH,
                )
            )
        return copies

    def finish_exchange(turn, copies):
        for delta in (-1, 0, 1):
            for shift in range(4):
                if delta == 0 and shift == 0:
                    continue
                slot = 4 * (1 - delta) + lax.rem(sub + shift, n_sub)
                pltpu.make_async_remote_copy(
                    src_ref=msg_ref.at[turn],
                    dst_ref=recv_ref.at[turn, slot],
                    send_sem=send_sem.at[turn, 0],
                    recv_sem=recv_sem.at[turn, slot],
                    device_id=(dom, lax.rem(sub + 1, n_sub)),
                    device_id_type=MESH,
                ).wait_recv()

    def local_part(table):
        return dot(pick_local, jnp.concatenate([stack2(table[0]), stack2(table[1])], axis=1))

    def beside_faces(turn, near):
        far = dot(pick_remote, stack2(recv_ref[turn].reshape(8 * SLOTS, 128)))
        faces = from_table(near[:, 0:128] + far[0:64], near[:, 128:256] + far[64:128])
        return jnp.concatenate(faces, axis=0).reshape(V, 8, 256)

    left = lhs3(first_half)
    faces = dot(left, pw_ref[...])
    table = to_table(faces)
    copies = start_exchange(0, table)
    pl.semaphore_wait(barrier, len(peers))
    for copy in copies:
        copy.start()
    sent = list(copies)

    loads[4].wait()
    spread(
        lambda v: jnp.concatenate([minus_ref[v, :, f, :] for f in range(4)], axis=1),
        4,
        32,
        J,
        cm_ref,
    )
    for i in (5, 9, 10):
        loads[i].wait()
    on_fault = jnp.concatenate([fault_faces_ref[f : f + 1, :] for f in range(4)], axis=1) == 1

    def coupling_row(v):
        plus = jnp.concatenate([plus_ref[v, :, f, :] for f in range(4)], axis=1)
        w_at = rows((V, 4 * E))
        friction = jnp.zeros((V, 4 * E), F32)
        for w in range(V):
            friction = jnp.where(w_at == w, fault_flux_ref[v, w], friction)
        return jnp.where(jnp.broadcast_to(on_fault, (V, 4 * E)), friction, plus)

    spread(coupling_row, 4, 32, J, cc_ref)

    def own_side(left, faces):
        volume = with_star(wv_ref, left)
        field = faces.reshape(V, 8, 256)
        for v in range(V):
            flux_ref[8 * v : 8 * v + 8, :] = contract(cm_ref, field, v)
        return volume

    def far_side(base, turn, near):
        field = beside_faces(turn, near)
        total = jnp.concatenate([contract(cc_ref, field, v) for v in range(V)], axis=0)
        return base - dot(lhs3(total + flux_ref[...]), pt3_ref[...])

    near = local_part(table)
    base = dofs + own_side(left, faces)
    finish_exchange(0, copies)
    moved = far_side(base, 0, near)

    again, _ = series(moved, False)
    carried = jnp.where(fine, again, second_half)
    left = lhs3(carried)
    faces = dot(left, pw_ref[...])
    table = to_table(faces)
    copies = start_exchange(1, table)
    for copy in copies:
        copy.start()
    sent += copies
    near = local_part(table)
    base = moved + own_side(left, faces)
    for copy in sent:
        copy.wait_send()
    finish_exchange(1, copies)
    after = far_side(base, 1, near)
    for v in range(V):
        out_ref[v, 0:8, :] = after[8 * v : 8 * v + 8, 0:M]
        out_ref[v, 8:16, :] = after[8 * v : 8 * v + 8, 64 : 64 + M]


def per_device(
    n_dom,
    n_sub,
    dofs,
    stiffness,
    projection,
    star,
    flux_minus,
    flux_plus,
    fault_flux,
    fault_faces,
    levels,
    face_source,
    send_source,
):
    vmem = pl.BlockSpec(memory_space=pltpu.VMEM)
    hbm = pl.BlockSpec(memory_space=pltpu.HBM)
    result = pl.pallas_call(
        functools.partial(kernel, n_dom, n_sub),
        out_shape=pltpu.VMEM((V, E, M), F32),
        in_specs=[hbm] * 11,
        out_specs=vmem,
        scratch_shapes=[
            pltpu.SMEM((E,), jnp.int32),
            pltpu.SMEM((4, E), jnp.int32),
            pltpu.SMEM((4,), jnp.int32),
            pltpu.SMEM((V, V), F32),
            pltpu.VMEM((4, E), jnp.int32),
            pltpu.VMEM((V, E, M), F32),
            pltpu.VMEM((3, M, M), F32),
            pltpu.VMEM((J, 4, M), F32),
            pltpu.VMEM((V, V, 3, E), F32),
            pltpu.VMEM((V, V, 4, E), F32),
            pltpu.VMEM((V, V, 4, E), F32),
            pltpu.VMEM((3, 128, 128), F32),
            pltpu.VMEM((256, 128), F32),
            pltpu.VMEM((72, 128), F32),
            pltpu.VMEM((V, 16, 128), F32),
            pltpu.VMEM((384, 384), BF16),
            pltpu.VMEM((384, 384), BF16),
            pltpu.VMEM((384, 256), BF16),
            pltpu.VMEM((768, 128), BF16),
            pltpu.VMEM((V, V, 8, 384), F32),
            pltpu.VMEM((V, V, 8, 256), F32),
            pltpu.VMEM((V, V, 8, 256), F32),
            pltpu.VMEM((72, 256), F32),
            pltpu.VMEM((2, 8, 128), F32),
            pltpu.VMEM((2, SLOTS, 8, 128), F32),
            pltpu.SemaphoreType.DMA((11,)),
            pltpu.SemaphoreType.DMA((2, SLOTS)),
            pltpu.SemaphoreType.DMA((2, SLOTS)),
        ],
        compiler_params=pltpu.CompilerParams(
            collective_id=0, has_side_effects=True, vmem_limit_bytes=VMEM_LIMIT
        ),
    )(
        *(
            pltpu.with_memory_space_constraint(x, pltpu.HBM)
            for x in (
        levels,
        face_source,
        send_source,
        fault_flux,
        fault_faces,
        jnp.transpose(dofs, (0, 2, 1)),
        stiffness,
        jnp.transpose(projection, (1, 0, 2)),
        jnp.transpose(star, (1, 2, 0, 3)),
        jnp.transpose(flux_minus, (1, 2, 0, 3)),
        jnp.transpose(flux_plus, (1, 2, 0, 3)),
                )
        )
    )
    return jnp.transpose(result, (0, 2, 1))


def solution(mesh):
    return jax.shard_map(
        functools.partial(per_device, mesh.shape["dom"], mesh.shape["sub"]),
        mesh=mesh,
        in_specs=(
            P(None, None, ("dom", "sub")),
            P(),
            P(),
            P(None, None, None, ("dom", "sub")),
            P(None, None, None, ("dom", "sub")),
            P(None, None, None, ("dom", "sub")),
            P(),
            P(None, ("dom", "sub")),
            P(("dom", "sub")),
            P(None, ("dom", "sub")),
            P(("dom", "sub")),
        ),
        out_specs=P(None, None, ("dom", "sub")),
        check_vma=False,
    )
```

```python
import functools
import math

import jax
import jax.numpy as jnp
from jax import lax
from jax.experimental import pallas as pl
from jax.experimental.pallas import tpu as pltpu
from jax.sharding import PartitionSpec as P

ORDER = 6
TAU = 0.75
V = 9
M = 56
J = 21
E = 16
SLOTS = 12
VMEM_LIMIT = 24 * 2**20
MESH = pl.DeviceIdType.MESH
F32 = jnp.float32
BF16 = jnp.bfloat16


def taylor_weights(start_time, stop_time):
    return [
        (stop_time ** (k + 1) - start_time ** (k + 1)) / math.factorial(k + 1)
        for k in range(ORDER)
    ]


FIRST = taylor_weights(0.0, TAU)
SECOND = taylor_weights(TAU, 2.0 * TAU)


def split(x):
    hi = x.astype(BF16)
    return hi, (x - hi.astype(F32)).astype(BF16)


def lhs3(x):
    hi, lo = split(x)
    return jnp.concatenate([hi, lo, hi], axis=1)


def rhs3(x):
    hi, lo = split(x)
    return jnp.concatenate([hi, hi, lo], axis=0)


def stack2(x):
    hi, lo = split(x)
    return jnp.concatenate([hi, lo], axis=0)


def dot(a, b):
    return jnp.dot(a, b, preferred_element_type=F32)


def lanes(shape=(8, 128)):
    return lax.broadcasted_iota(jnp.int32, shape, 1)


def rows(shape=(8, 128)):
    return lax.broadcasted_iota(jnp.int32, shape, 0)


def roll(x, shift):
    return pltpu.roll(x, shift % 128, 1)


def swap_blocks(a):
    lane = lanes()
    low = lane < 64
    even = (lane // 32) % 2 == 0
    p0 = jnp.where(low, a[0], roll(a[2], 64))
    p2 = jnp.where(low, roll(a[0], 64), a[2])
    p1 = jnp.where(low, a[1], roll(a[3], 64))
    p3 = jnp.where(low, roll(a[1], 64), a[3])
    return [
        jnp.where(even, p0, roll(p1, 32)),
        jnp.where(even, roll(p0, -32), p1),
        jnp.where(even, p2, roll(p3, 32)),
        jnp.where(even, roll(p2, -32), p3),
    ]


def to_table(faces):
    lane = lanes()
    ends = (lane >= J) & (lane < 32)
    more = (lane >= 32 + J) & (lane < 42 + J)
    first, second = [], []
    for half in range(2):
        part = [faces[8 * w : 8 * w + 8, 128 * half : 128 * half + 128] for w in range(V)]
        one = swap_blocks(part[0:4])
        two = swap_blocks(part[4:8])
        for b in range(4):
            kept = jnp.where(ends, roll(part[8], J - 32 * b), one[b])
            first.append(jnp.where(more, roll(part[8], 42 - 32 * b), kept))
            second.append(two[b])
    return jnp.concatenate(first, axis=0), jnp.concatenate(second, axis=0)


def from_table(first, second):
    lane = lanes()
    halves = []
    for half in range(2):
        one = [first[32 * half + 8 * b : 32 * half + 8 * b + 8] for b in range(4)]
        two = [second[32 * half + 8 * b : 32 * half + 8 * b + 8] for b in range(4)]
        last = jnp.zeros((8, 128), F32)
        for b in range(4):
            inside = lane - 32 * b
            last = jnp.where((inside >= 0) & (inside < 11), roll(one[b], 32 * b - J), last)
            last = jnp.where((inside >= 11) & (inside < J), roll(one[b], 32 * b - 42), last)
        halves.append(swap_blocks(one) + swap_blocks(two) + [last])
    return [jnp.concatenate([halves[0][w], halves[1][w]], axis=1) for w in range(V)]


def kernel(
    n_dom,
    n_sub,
    levels_hbm,
    source_hbm,
    send_hbm,
    fault_flux_hbm,
    fault_faces_hbm,
    dofs_hbm,
    stiff_hbm,
    proj_hbm,
    star_hbm,
    minus_hbm,
    plus_hbm,
    out_ref,
    levels_ref,
    source_ref,
    send_ref,
    fault_flux_ref,
    fault_faces_ref,
    dofs_ref,
    stiff_ref,
    proj_ref,
    star_ref,
    minus_ref,
    plus_ref,
    block_ref,
    pt_ref,
    x_ref,
    row_ref,
    wd_ref,
    wv_ref,
    pw_ref,
    pt3_ref,
    cs_ref,
    cm_ref,
    cc_ref,
    flux_ref,
    msg_ref,
    recv_ref,
    in_sem,
    send_sem,
    recv_sem,
):
    dom = lax.axis_index("dom")
    sub = lax.axis_index("sub")
    peers = []
    for delta in (-1, 1, 0):
        for turn in (2, 1, 3, 0):
            if delta == 0 and turn == 0:
                continue
            peers.append((delta, lax.rem(dom + delta + n_dom, n_dom), lax.rem(sub + turn, n_sub)))

    barrier = pltpu.get_barrier_semaphore()
    for _, to_dom, to_sub in peers:
        pl.semaphore_signal(barrier, inc=1, device_id=(to_dom, to_sub), device_id_type=MESH)

    loads = [
        pltpu.make_async_copy(src, dst, in_sem.at[i])
        for i, (src, dst) in enumerate(
            (
                (stiff_hbm, stiff_ref),
                (star_hbm, star_ref),
                (dofs_hbm, dofs_ref),
                (proj_hbm, proj_ref),
                (minus_hbm, minus_ref),
                (plus_hbm, plus_ref),
                (levels_hbm, levels_ref),
                (source_hbm, source_ref),
                (send_hbm, send_ref),
                (fault_flux_hbm, fault_flux_ref),
                (fault_faces_hbm, fault_faces_ref),
            )
        )
    ]
    for load in loads:
        load.start()

    block_ref[...] = jnp.zeros(block_ref.shape, F32)
    pt_ref[...] = jnp.zeros(pt_ref.shape, F32)
    x_ref[...] = jnp.zeros(x_ref.shape, F32)
    row_ref[...] = jnp.zeros(row_ref.shape, F32)

    loads[0].wait()
    for d in range(3):
        block_ref[d, 0:M, 0:M] = stiff_ref[d]
        block_ref[d, 64 : 64 + M, 64 : 64 + M] = stiff_ref[d]
    for d in range(3):
        block = block_ref[d]
        wd_ref[:, 128 * d : 128 * d + 128] = rhs3(block.T)
        wv_ref[:, 128 * d : 128 * d + 128] = rhs3(block)

    def spread(make_row, groups, part_width, fill, coef_ref):
        width = 128 * coef_ref.shape[3] // 128
        k = lax.broadcasted_iota(jnp.int32, (128, width), 0) % 64
        lane = lax.broadcasted_iota(jnp.int32, (128, width), 1)
        group = lane // (2 * part_width)
        half = (lane // part_width) % 2
        hit = (k // E == group) & ((k % E) // 8 == half) & (lane % part_width < fill)
        repeat = hit.astype(F32).astype(BF16)
        keep = (lanes() % 8 == rows()).astype(F32)
        for v in range(V):
            row = make_row(v)
            high = row.astype(BF16).astype(F32)
            row_ref[v, 0:V, 0 : groups * E] = high
            row_ref[v, 0:V, 64 : 64 + groups * E] = row - high
        for v in range(V):
            left = jnp.concatenate(
                [jnp.broadcast_to(row_ref[v, w : w + 1, :], (8, 128)) * keep for w in range(V)],
                axis=0,
            ).astype(BF16)
            coef_ref[v] = dot(left, repeat).reshape(V, 8, width)

    loads[1].wait()
    spread(
        lambda v: jnp.concatenate([star_ref[v, :, d, :] for d in range(3)], axis=1),
        3,
        64,
        M,
        cs_ref,
    )

    loads[2].wait()
    for v in range(V):
        x_ref[8 * v : 8 * v + 8, 0:M] = dofs_ref[v, 0:8, :]
        x_ref[8 * v : 8 * v + 8, 64 : 64 + M] = dofs_ref[v, 8:16, :]

    def contract(coef_ref, field, v):
        return (coef_ref[v] * field).sum(axis=0)

    def with_star(weights_ref, left):
        field = dot(left, weights_ref[...]).reshape(V, 8, 384)
        result = []
        for v in range(V):
            total = contract(cs_ref, field, v)
            result.append(total[:, 0:128] + total[:, 128:256] + total[:, 256:384])
        return jnp.concatenate(result, axis=0)

    def series(start, want_second):
        current = start
        first = FIRST[0] * current
        second = SECOND[0] * current if want_second else None
        for k in range(1, ORDER):
            current = with_star(wd_ref, lhs3(current))
            first = first + FIRST[k] * current
            if want_second:
                second = second + SECOND[k] * current
        return first, second

    loads[3].wait()
    for f in range(4):
        for half in range(2):
            at = 64 * f + 32 * half
            pt_ref[at : at + J, 64 * half : 64 * half + M] = proj_ref[:, f, :]
    pt = pt_ref[...]
    pw_ref[...] = rhs3(pt.T)
    pt3_ref[...] = rhs3(pt)

    for i in (6, 7, 8):
        loads[i].wait()
    row = rows((8, 256))
    lane = lanes((8, 256))
    wanted = jnp.full((8, 256), -1, jnp.int32)
    for s in range(4):
        wanted = jnp.where(row % 4 == s, send_ref[s], wanted)
    pick_send = ((lane % 64 == wanted) & (lane // 128 == row // 4)).astype(F32).astype(BF16)

    local_rows, remote_rows = [], []
    row = rows()
    lane = lanes()
    lane2 = lanes((8, 192)) % 96
    for f in range(4):
        for half in range(2):
            wanted = jnp.full((8, 128), -1, jnp.int32)
            for i in range(8):
                wanted = jnp.where(row == i, source_ref[f, 8 * half + i], wanted)
            local_rows.append((lane % 64 == wanted).astype(F32))
            far = wanted - 64
            code = jnp.where(far >= 0, (far // 4) * 8 + far % 4, -8)
            code = jnp.concatenate([code, code[:, 0:64]], axis=1)
            remote_rows.append((code, lane2))
    pick_local = jnp.concatenate(local_rows, axis=0).astype(BF16)
    pick_remote = jnp.concatenate(
        [(at == code + 4 * q).astype(F32) for q in range(2) for code, at in remote_rows], axis=0
    ).astype(BF16)

    fine = jnp.zeros((8, 128), jnp.int32)
    for e in range(E):
        here = (row == e % 8) & (lane // 64 == e // 8)
        fine = jnp.where(here & (levels_ref[e] == 0), 1, fine)
    fine = jnp.concatenate([fine] * V, axis=0) == 1

    dofs = x_ref[...]
    first_half, second_half = series(dofs, True)

    def start_exchange(turn, table):
        stacked = jnp.concatenate([stack2(table[0]), stack2(table[1])], axis=0)
        message = dot(pick_send, stacked)
        msg_ref[turn] = message
        recv_ref[turn, 4 + sub] = message
        return [
            pltpu.make_async_remote_copy(
                src_ref=msg_ref.at[turn],
                dst_ref=recv_ref.at[turn, 4 * (1 - delta) + sub],
                send_sem=send_sem.at[turn],
                recv_sem=recv_sem.at[turn],
                device_id=(to_dom, to_sub),
                device_id_type=MESH,
            )
            for delta, to_dom, to_sub in peers
        ]

    def all_messages(turn):
        some = recv_ref.at[turn, pl.ds(0, len(peers))]
        return pltpu.make_async_remote_copy(
            src_ref=some,
            dst_ref=some,
            send_sem=send_sem.at[turn],
            recv_sem=recv_sem.at[turn],
            device_id=(dom, lax.rem(sub + 1, n_sub)),
            device_id_type=MESH,
        )

    def finish_exchange(turn, copies):
        all_messages(turn).wait_recv()

    def local_part(table):
        return dot(pick_local, jnp.concatenate([stack2(table[0]), stack2(table[1])], axis=1))

    def beside_faces(turn, near):
        far = dot(pick_remote, stack2(recv_ref[turn].reshape(8 * SLOTS, 128)))
        faces = from_table(near[:, 0:128] + far[0:64], near[:, 128:256] + far[64:128])
        return jnp.concatenate(faces, axis=0).reshape(V, 8, 256)

    left = lhs3(first_half)
    faces = dot(left, pw_ref[...])
    table = to_table(faces)
    copies = start_exchange(0, table)
    pl.semaphore_wait(barrier, len(peers))
    for copy in copies:
        copy.start()

    loads[4].wait()
    spread(
        lambda v: jnp.concatenate([minus_ref[v, :, f, :] for f in range(4)], axis=1),
        4,
        32,
        J,
        cm_ref,
    )
    for i in (5, 9, 10):
        loads[i].wait()
    on_fault = jnp.concatenate([fault_faces_ref[f : f + 1, :] for f in range(4)], axis=1) == 1

    def coupling_row(v):
        plus = jnp.concatenate([plus_ref[v, :, f, :] for f in range(4)], axis=1)
        w_at = rows((V, 4 * E))
        friction = jnp.zeros((V, 4 * E), F32)
        for w in range(V):
            friction = jnp.where(w_at == w, fault_flux_ref[v, w], friction)
        return jnp.where(jnp.broadcast_to(on_fault, (V, 4 * E)), friction, plus)

    spread(coupling_row, 4, 32, J, cc_ref)

    def own_side(left, faces):
        volume = with_star(wv_ref, left)
        field = faces.reshape(V, 8, 256)
        for v in range(V):
            flux_ref[8 * v : 8 * v + 8, :] = contract(cm_ref, field, v)
        return volume

    def far_side(base, turn, near):
        field = beside_faces(turn, near)
        total = jnp.concatenate([contract(cc_ref, field, v) for v in range(V)], axis=0)
        return base - dot(lhs3(total + flux_ref[...]), pt3_ref[...])

    near = local_part(table)
    base = dofs + own_side(left, faces)
    finish_exchange(0, copies)
    moved = far_side(base, 0, near)

    again, _ = series(moved, False)
    carried = jnp.where(fine, again, second_half)
    left = lhs3(carried)
    faces = dot(left, pw_ref[...])
    table = to_table(faces)
    copies = start_exchange(1, table)
    for copy in copies:
        copy.start()
    near = local_part(table)
    base = moved + own_side(left, faces)
    all_messages(0).wait_send()
    all_messages(1).wait_send()
    finish_exchange(1, copies)
    after = far_side(base, 1, near)
    for v in range(V):
        out_ref[v, 0:8, :] = after[8 * v : 8 * v + 8, 0:M]
        out_ref[v, 8:16, :] = after[8 * v : 8 * v + 8, 64 : 64 + M]


def per_device(
    n_dom,
    n_sub,
    dofs,
    stiffness,
    projection,
    star,
    flux_minus,
    flux_plus,
    fault_flux,
    fault_faces,
    levels,
    face_source,
    send_source,
):
    vmem = pl.BlockSpec(memory_space=pltpu.VMEM)
    hbm = pl.BlockSpec(memory_space=pltpu.HBM)
    result = pl.pallas_call(
        functools.partial(kernel, n_dom, n_sub),
        out_shape=pltpu.VMEM((V, E, M), F32),
        in_specs=[hbm] * 11,
        out_specs=vmem,
        scratch_shapes=[
            pltpu.SMEM((E,), jnp.int32),
            pltpu.SMEM((4, E), jnp.int32),
            pltpu.SMEM((4,), jnp.int32),
            pltpu.SMEM((V, V), F32),
            pltpu.VMEM((4, E), jnp.int32),
            pltpu.VMEM((V, E, M), F32),
            pltpu.VMEM((3, M, M), F32),
            pltpu.VMEM((J, 4, M), F32),
            pltpu.VMEM((V, V, 3, E), F32),
            pltpu.VMEM((V, V, 4, E), F32),
            pltpu.VMEM((V, V, 4, E), F32),
            pltpu.VMEM((3, 128, 128), F32),
            pltpu.VMEM((256, 128), F32),
            pltpu.VMEM((72, 128), F32),
            pltpu.VMEM((V, 16, 128), F32),
            pltpu.VMEM((384, 384), BF16),
            pltpu.VMEM((384, 384), BF16),
            pltpu.VMEM((384, 256), BF16),
            pltpu.VMEM((768, 128), BF16),
            pltpu.VMEM((V, V, 8, 384), F32),
            pltpu.VMEM((V, V, 8, 256), F32),
            pltpu.VMEM((V, V, 8, 256), F32),
            pltpu.VMEM((72, 256), F32),
            pltpu.VMEM((2, 8, 128), F32),
            pltpu.VMEM((2, SLOTS, 8, 128), F32),
            pltpu.SemaphoreType.DMA((11,)),
            pltpu.SemaphoreType.DMA((2,)),
            pltpu.SemaphoreType.DMA((2,)),
        ],
        compiler_params=pltpu.CompilerParams(
            collective_id=0, has_side_effects=True, vmem_limit_bytes=VMEM_LIMIT
        ),
    )(
        *(
            pltpu.with_memory_space_constraint(x, pltpu.HBM)
            for x in (
        levels,
        face_source,
        send_source,
        fault_flux,
        fault_faces,
        jnp.transpose(dofs, (0, 2, 1)),
        stiffness,
        jnp.transpose(projection, (1, 0, 2)),
        jnp.transpose(star, (1, 2, 0, 3)),
        jnp.transpose(flux_minus, (1, 2, 0, 3)),
        jnp.transpose(flux_plus, (1, 2, 0, 3)),
                )
        )
    )
    return jnp.transpose(result, (0, 2, 1))


def solution(mesh):
    return jax.shard_map(
        functools.partial(per_device, mesh.shape["dom"], mesh.shape["sub"]),
        mesh=mesh,
        in_specs=(
            P(None, None, ("dom", "sub")),
            P(),
            P(),
            P(None, None, None, ("dom", "sub")),
            P(None, None, None, ("dom", "sub")),
            P(None, None, None, ("dom", "sub")),
            P(),
            P(None, ("dom", "sub")),
            P(("dom", "sub")),
            P(None, ("dom", "sub")),
            P(("dom", "sub")),
        ),
        out_specs=P(None, None, ("dom", "sub")),
        check_vma=False,
    )
```

```python
import functools
import math

import jax
import jax.numpy as jnp
from jax import lax
from jax.experimental import pallas as pl
from jax.experimental.pallas import tpu as pltpu
from jax.sharding import PartitionSpec as P

ORDER = 6
TAU = 0.75
V = 9
M = 56
J = 21
E = 16
SLOTS = 12
VMEM_LIMIT = 24 * 2**20
FARTHEST_FIRST = (
    (-1, 2),
    (1, 2),
    (-1, 1),
    (1, 1),
    (-1, 3),
    (1, 3),
    (0, 2),
    (-1, 0),
    (1, 0),
    (0, 1),
    (0, 3),
)
MESH = pl.DeviceIdType.MESH
F32 = jnp.float32
BF16 = jnp.bfloat16


def taylor_weights(start_time, stop_time):
    return [
        (stop_time ** (k + 1) - start_time ** (k + 1)) / math.factorial(k + 1)
        for k in range(ORDER)
    ]


FIRST = taylor_weights(0.0, TAU)
SECOND = taylor_weights(TAU, 2.0 * TAU)


def split(x):
    hi = x.astype(BF16)
    return hi, (x - hi.astype(F32)).astype(BF16)


def lhs3(x):
    hi, lo = split(x)
    return jnp.concatenate([hi, lo, hi], axis=1)


def rhs3(x):
    hi, lo = split(x)
    return jnp.concatenate([hi, hi, lo], axis=0)


def stack2(x):
    hi, lo = split(x)
    return jnp.concatenate([hi, lo], axis=0)


def dot(a, b):
    return jnp.dot(a, b, preferred_element_type=F32)


def lanes(shape=(8, 128)):
    return lax.broadcasted_iota(jnp.int32, shape, 1)


def rows(shape=(8, 128)):
    return lax.broadcasted_iota(jnp.int32, shape, 0)


def roll(x, shift):
    return pltpu.roll(x, shift % 128, 1)


def swap_blocks(a):
    lane = lanes()
    low = lane < 64
    even = (lane // 32) % 2 == 0
    p0 = jnp.where(low, a[0], roll(a[2], 64))
    p2 = jnp.where(low, roll(a[0], 64), a[2])
    p1 = jnp.where(low, a[1], roll(a[3], 64))
    p3 = jnp.where(low, roll(a[1], 64), a[3])
    return [
        jnp.where(even, p0, roll(p1, 32)),
        jnp.where(even, roll(p0, -32), p1),
        jnp.where(even, p2, roll(p3, 32)),
        jnp.where(even, roll(p2, -32), p3),
    ]


def to_table(faces):
    lane = lanes()
    ends = (lane >= J) & (lane < 32)
    more = (lane >= 32 + J) & (lane < 42 + J)
    first, second = [], []
    for half in range(2):
        part = [faces[8 * w : 8 * w + 8, 128 * half : 128 * half + 128] for w in range(V)]
        one = swap_blocks(part[0:4])
        two = swap_blocks(part[4:8])
        for b in range(4):
            kept = jnp.where(ends, roll(part[8], J - 32 * b), one[b])
            first.append(jnp.where(more, roll(part[8], 42 - 32 * b), kept))
            second.append(two[b])
    return jnp.concatenate(first, axis=0), jnp.concatenate(second, axis=0)


def from_table(first, second):
    lane = lanes()
    halves = []
    for half in range(2):
        one = [first[32 * half + 8 * b : 32 * half + 8 * b + 8] for b in range(4)]
        two = [second[32 * half + 8 * b : 32 * half + 8 * b + 8] for b in range(4)]
        last = jnp.zeros((8, 128), F32)
        for b in range(4):
            inside = lane - 32 * b
            last = jnp.where((inside >= 0) & (inside < 11), roll(one[b], 32 * b - J), last)
            last = jnp.where((inside >= 11) & (inside < J), roll(one[b], 32 * b - 42), last)
        halves.append(swap_blocks(one) + swap_blocks(two) + [last])
    return [jnp.concatenate([halves[0][w], halves[1][w]], axis=1) for w in range(V)]


def kernel(
    n_dom,
    n_sub,
    levels_hbm,
    source_hbm,
    send_hbm,
    fault_flux_hbm,
    fault_faces_hbm,
    dofs_hbm,
    stiff_hbm,
    proj_hbm,
    star_hbm,
    minus_hbm,
    plus_hbm,
    out_ref,
    levels_ref,
    source_ref,
    send_ref,
    fault_flux_ref,
    fault_faces_ref,
    dofs_ref,
    stiff_ref,
    proj_ref,
    star_ref,
    minus_ref,
    plus_ref,
    block_ref,
    pt_ref,
    x_ref,
    row_ref,
    wd_ref,
    wv_ref,
    pw_ref,
    pt3_ref,
    ptw_ref,
    cs_ref,
    cm_ref,
    cc_ref,
    flux_ref,
    msg_ref,
    recv_ref,
    in_sem,
    send_sem,
    recv_sem,
):
    dom = lax.axis_index("dom")
    sub = lax.axis_index("sub")
    peers = []
    for delta, turn in FARTHEST_FIRST:
        peers.append((delta, lax.rem(dom + delta + n_dom, n_dom), lax.rem(sub + turn, n_sub)))

    barrier = pltpu.get_barrier_semaphore()
    for _, to_dom, to_sub in peers:
        pl.semaphore_signal(barrier, inc=1, device_id=(to_dom, to_sub), device_id_type=MESH)

    loads = [
        pltpu.make_async_copy(src, dst, in_sem.at[i])
        for i, (src, dst) in enumerate(
            (
                (stiff_hbm, stiff_ref),
                (star_hbm, star_ref),
                (dofs_hbm, dofs_ref),
                (proj_hbm, proj_ref),
                (minus_hbm, minus_ref),
                (plus_hbm, plus_ref),
                (levels_hbm, levels_ref),
                (source_hbm, source_ref),
                (send_hbm, send_ref),
                (fault_flux_hbm, fault_flux_ref),
                (fault_faces_hbm, fault_faces_ref),
            )
        )
    ]
    for load in loads:
        load.start()

    block_ref[...] = jnp.zeros(block_ref.shape, F32)
    pt_ref[...] = jnp.zeros(pt_ref.shape, F32)
    x_ref[...] = jnp.zeros(x_ref.shape, F32)
    row_ref[...] = jnp.zeros(row_ref.shape, F32)

    loads[0].wait()
    for d in range(3):
        block_ref[d, 0:M, 0:M] = stiff_ref[d]
        block_ref[d, 64 : 64 + M, 64 : 64 + M] = stiff_ref[d]
    for d in range(3):
        block = block_ref[d]
        wd_ref[:, 128 * d : 128 * d + 128] = rhs3(block.T)
        wv_ref[:, 128 * d : 128 * d + 128] = rhs3(block)

    def spread(make_row, groups, part_width, fill, coef_ref):
        width = 128 * coef_ref.shape[3] // 128
        k = lax.broadcasted_iota(jnp.int32, (128, width), 0) % 64
        lane = lax.broadcasted_iota(jnp.int32, (128, width), 1)
        group = lane // (2 * part_width)
        half = (lane // part_width) % 2
        hit = (k // E == group) & ((k % E) // 8 == half) & (lane % part_width < fill)
        repeat = hit.astype(F32).astype(BF16)
        keep = (lanes() % 8 == rows()).astype(F32)
        for v in range(V):
            row = make_row(v)
            high = row.astype(BF16).astype(F32)
            row_ref[v, 0:V, 0 : groups * E] = high
            row_ref[v, 0:V, 64 : 64 + groups * E] = row - high
        for v in range(V):
            left = jnp.concatenate(
                [jnp.broadcast_to(row_ref[v, w : w + 1, :], (8, 128)) * keep for w in range(V)],
                axis=0,
            ).astype(BF16)
            coef_ref[v] = dot(left, repeat).reshape(V, 8, width)

    loads[1].wait()
    spread(
        lambda v: jnp.concatenate([star_ref[v, :, d, :] for d in range(3)], axis=1),
        3,
        64,
        M,
        cs_ref,
    )

    loads[2].wait()
    for v in range(V):
        x_ref[8 * v : 8 * v + 8, 0:M] = dofs_ref[v, 0:8, :]
        x_ref[8 * v : 8 * v + 8, 64 : 64 + M] = dofs_ref[v, 8:16, :]

    def contract(coef_ref, field, v):
        return (coef_ref[v] * field).sum(axis=0)

    def with_star(weights_ref, left):
        return star_sum(dot(left, weights_ref[...]))

    def star_sum(field):
        field = field.reshape(V, 8, 384)
        result = []
        for v in range(V):
            total = contract(cs_ref, field, v)
            result.append(total[:, 0:128] + total[:, 128:256] + total[:, 256:384])
        return jnp.concatenate(result, axis=0)

    def series(start, want_second, opening=None):
        current = start
        first = FIRST[0] * current
        second = SECOND[0] * current if want_second else None
        for k in range(1, ORDER):
            if k == 1 and opening is not None:
                current = star_sum(opening)
            else:
                current = with_star(wd_ref, lhs3(current))
            first = first + FIRST[k] * current
            if want_second:
                second = second + SECOND[k] * current
        return first, second

    loads[3].wait()
    for f in range(4):
        for half in range(2):
            at = 64 * f + 32 * half
            pt_ref[at : at + J, 64 * half : 64 * half + M] = proj_ref[:, f, :]
    pt = pt_ref[...]
    pw_ref[...] = rhs3(pt.T)
    pt3_ref[...] = rhs3(pt)

    for i in (6, 7, 8):
        loads[i].wait()
    row = rows((8, 256))
    lane = lanes((8, 256))
    wanted = jnp.full((8, 256), -1, jnp.int32)
    for s in range(4):
        wanted = jnp.where(row % 4 == s, send_ref[s], wanted)
    pick_send = ((lane % 64 == wanted) & (lane // 128 == row // 4)).astype(F32).astype(BF16)

    local_rows, remote_rows = [], []
    row = rows()
    lane = lanes()
    lane2 = lanes((8, 192)) % 96
    for f in range(4):
        for half in range(2):
            wanted = jnp.full((8, 128), -1, jnp.int32)
            for i in range(8):
                wanted = jnp.where(row == i, source_ref[f, 8 * half + i], wanted)
            local_rows.append((lane % 64 == wanted).astype(F32))
            far = wanted - 64
            code = jnp.where(far >= 0, (far // 4) * 8 + far % 4, -8)
            code = jnp.concatenate([code, code[:, 0:64]], axis=1)
            remote_rows.append((code, lane2))
    pick_local = jnp.concatenate(local_rows, axis=0).astype(BF16)
    pick_remote = jnp.concatenate(
        [(at == code + 4 * q).astype(F32) for q in range(2) for code, at in remote_rows], axis=0
    ).astype(BF16)

    fine = jnp.zeros((8, 128), jnp.int32)
    for e in range(E):
        here = (row == e % 8) & (lane // 64 == e // 8)
        fine = jnp.where(here & (levels_ref[e] == 0), 1, fine)
    fine = jnp.concatenate([fine] * V, axis=0) == 1

    dofs = x_ref[...]
    first_half, second_half = series(dofs, True)

    def start_exchange(turn, table):
        stacked = jnp.concatenate([stack2(table[0]), stack2(table[1])], axis=0)
        message = dot(pick_send, stacked)
        msg_ref[turn] = message
        recv_ref[turn, 4 + sub] = message
        return [
            pltpu.make_async_remote_copy(
                src_ref=msg_ref.at[turn],
                dst_ref=recv_ref.at[turn, 4 * (1 - delta) + sub],
                send_sem=send_sem.at[turn],
                recv_sem=recv_sem.at[turn],
                device_id=(to_dom, to_sub),
                device_id_type=MESH,
            )
            for delta, to_dom, to_sub in peers
        ]

    def all_messages(turn):
        some = recv_ref.at[turn, pl.ds(0, len(peers))]
        return pltpu.make_async_remote_copy(
            src_ref=some,
            dst_ref=some,
            send_sem=send_sem.at[turn],
            recv_sem=recv_sem.at[turn],
            device_id=(dom, lax.rem(sub + 1, n_sub)),
            device_id_type=MESH,
        )

    def finish_exchange(turn, copies):
        all_messages(turn).wait_recv()

    def local_part(table):
        return dot(pick_local, jnp.concatenate([stack2(table[0]), stack2(table[1])], axis=1))

    def beside_faces(turn, near):
        arrived = stack2(recv_ref[turn].reshape(8 * SLOTS, 128))
        faces = from_table(
            near[:, 0:128] + dot(pick_remote[0:64], arrived),
            near[:, 128:256] + dot(pick_remote[64:128], arrived),
        )
        return jnp.concatenate(faces, axis=0).reshape(V, 8, 256)

    left = lhs3(first_half)
    faces = dot(left, pw_ref[...])
    table = to_table(faces)
    copies = start_exchange(0, table)
    pl.semaphore_wait(barrier, len(peers))
    for copy in copies:
        copy.start()

    loads[4].wait()
    spread(
        lambda v: jnp.concatenate([minus_ref[v, :, f, :] for f in range(4)], axis=1),
        4,
        32,
        J,
        cm_ref,
    )
    for i in (5, 9, 10):
        loads[i].wait()
    on_fault = jnp.concatenate([fault_faces_ref[f : f + 1, :] for f in range(4)], axis=1) == 1

    def coupling_row(v):
        plus = jnp.concatenate([plus_ref[v, :, f, :] for f in range(4)], axis=1)
        w_at = rows((V, 4 * E))
        friction = jnp.zeros((V, 4 * E), F32)
        for w in range(V):
            friction = jnp.where(w_at == w, fault_flux_ref[v, w], friction)
        return jnp.where(jnp.broadcast_to(on_fault, (V, 4 * E)), friction, plus)

    spread(coupling_row, 4, 32, J, cc_ref)

    def own_side(left, faces):
        volume = with_star(wv_ref, left)
        field = faces.reshape(V, 8, 256)
        for v in range(V):
            flux_ref[8 * v : 8 * v + 8, :] = contract(cm_ref, field, v)
        return volume

    def fluxes(turn, near):
        field = beside_faces(turn, near)
        total = jnp.concatenate([contract(cc_ref, field, v) for v in range(V)], axis=0)
        hi, lo = split(total + flux_ref[...])
        return jnp.concatenate([hi, lo], axis=1), hi

    near = local_part(table)
    base = dofs + own_side(left, faces)
    base_slopes = dot(lhs3(base), wd_ref[...])
    ptw_ref[...] = rhs3(dot(lhs3(pt), wd_ref[...]))
    finish_exchange(0, copies)
    both, hi = fluxes(0, near)
    opening = base_slopes - dot(both, ptw_ref[0:512, :]) - dot(hi, ptw_ref[512:768, :])
    moved = base - dot(both, pt3_ref[0:512, :]) - dot(hi, pt3_ref[512:768, :])

    again, _ = series(moved, False, opening)
    carried = jnp.where(fine, again, second_half)
    left = lhs3(carried)
    faces = dot(left, pw_ref[...])
    table = to_table(faces)
    copies = start_exchange(1, table)
    for copy in copies:
        copy.start()
    near = local_part(table)
    base = moved + own_side(left, faces)
    all_messages(0).wait_send()
    all_messages(1).wait_send()
    finish_exchange(1, copies)
    both, hi = fluxes(1, near)
    after = base - dot(both, pt3_ref[0:512, :]) - dot(hi, pt3_ref[512:768, :])
    for v in range(V):
        out_ref[v, 0:8, :] = after[8 * v : 8 * v + 8, 0:M]
        out_ref[v, 8:16, :] = after[8 * v : 8 * v + 8, 64 : 64 + M]


def per_device(
    n_dom,
    n_sub,
    dofs,
    stiffness,
    projection,
    star,
    flux_minus,
    flux_plus,
    fault_flux,
    fault_faces,
    levels,
    face_source,
    send_source,
):
    vmem = pl.BlockSpec(memory_space=pltpu.VMEM)
    hbm = pl.BlockSpec(memory_space=pltpu.HBM)
    result = pl.pallas_call(
        functools.partial(kernel, n_dom, n_sub),
        out_shape=pltpu.VMEM((V, E, M), F32),
        in_specs=[hbm] * 11,
        out_specs=vmem,
        scratch_shapes=[
            pltpu.SMEM((E,), jnp.int32),
            pltpu.SMEM((4, E), jnp.int32),
            pltpu.SMEM((4,), jnp.int32),
            pltpu.SMEM((V, V), F32),
            pltpu.VMEM((4, E), jnp.int32),
            pltpu.VMEM((V, E, M), F32),
            pltpu.VMEM((3, M, M), F32),
            pltpu.VMEM((J, 4, M), F32),
            pltpu.VMEM((V, V, 3, E), F32),
            pltpu.VMEM((V, V, 4, E), F32),
            pltpu.VMEM((V, V, 4, E), F32),
            pltpu.VMEM((3, 128, 128), F32),
            pltpu.VMEM((256, 128), F32),
            pltpu.VMEM((72, 128), F32),
            pltpu.VMEM((V, 16, 128), F32),
            pltpu.VMEM((384, 384), BF16),
            pltpu.VMEM((384, 384), BF16),
            pltpu.VMEM((384, 256), BF16),
            pltpu.VMEM((768, 128), BF16),
            pltpu.VMEM((768, 384), BF16),
            pltpu.VMEM((V, V, 8, 384), F32),
            pltpu.VMEM((V, V, 8, 256), F32),
            pltpu.VMEM((V, V, 8, 256), F32),
            pltpu.VMEM((72, 256), F32),
            pltpu.VMEM((2, 8, 128), F32),
            pltpu.VMEM((2, SLOTS, 8, 128), F32),
            pltpu.SemaphoreType.DMA((11,)),
            pltpu.SemaphoreType.DMA((2,)),
            pltpu.SemaphoreType.DMA((2,)),
        ],
        compiler_params=pltpu.CompilerParams(
            collective_id=0, has_side_effects=True, vmem_limit_bytes=VMEM_LIMIT
        ),
    )(
        *(
            pltpu.with_memory_space_constraint(x, pltpu.HBM)
            for x in (
        levels,
        face_source,
        send_source,
        fault_flux,
        fault_faces,
        jnp.transpose(dofs, (0, 2, 1)),
        stiffness,
        jnp.transpose(projection, (1, 0, 2)),
        jnp.transpose(star, (1, 2, 0, 3)),
        jnp.transpose(flux_minus, (1, 2, 0, 3)),
        jnp.transpose(flux_plus, (1, 2, 0, 3)),
                )
        )
    )
    return jnp.transpose(result, (0, 2, 1))


def solution(mesh):
    return jax.shard_map(
        functools.partial(per_device, mesh.shape["dom"], mesh.shape["sub"]),
        mesh=mesh,
        in_specs=(
            P(None, None, ("dom", "sub")),
            P(),
            P(),
            P(None, None, None, ("dom", "sub")),
            P(None, None, None, ("dom", "sub")),
            P(None, None, None, ("dom", "sub")),
            P(),
            P(None, ("dom", "sub")),
            P(("dom", "sub")),
            P(None, ("dom", "sub")),
            P(("dom", "sub")),
        ),
        out_specs=P(None, None, ("dom", "sub")),
        check_vma=False,
    )
```

```python
import functools
import math

import jax
import jax.numpy as jnp
from jax import lax
from jax.experimental import pallas as pl
from jax.experimental.pallas import tpu as pltpu
from jax.sharding import PartitionSpec as P

ORDER = 6
TAU = 0.75
V = 9
M = 56
J = 21
E = 16
SLOTS = 12
VMEM_LIMIT = 24 * 2**20
FARTHEST_FIRST = (
    (-1, 2),
    (1, 2),
    (-1, 1),
    (1, 1),
    (-1, 3),
    (1, 3),
    (0, 2),
    (-1, 0),
    (1, 0),
    (0, 1),
    (0, 3),
)
MESH = pl.DeviceIdType.MESH
F32 = jnp.float32
BF16 = jnp.bfloat16


def taylor_weights(start_time, stop_time):
    return [
        (stop_time ** (k + 1) - start_time ** (k + 1)) / math.factorial(k + 1)
        for k in range(ORDER)
    ]


FIRST = taylor_weights(0.0, TAU)
SECOND = taylor_weights(TAU, 2.0 * TAU)


def split(x):
    hi = x.astype(BF16)
    return hi, (x - hi.astype(F32)).astype(BF16)


def lhs3(x):
    hi, lo = split(x)
    return jnp.concatenate([hi, lo, hi], axis=1)


def rhs3(x):
    hi, lo = split(x)
    return jnp.concatenate([hi, hi, lo], axis=0)


def stack2(x):
    hi, lo = split(x)
    return jnp.concatenate([hi, lo], axis=0)


def dot(a, b):
    return jnp.dot(a, b, preferred_element_type=F32)


def lanes(shape=(8, 128)):
    return lax.broadcasted_iota(jnp.int32, shape, 1)


def rows(shape=(8, 128)):
    return lax.broadcasted_iota(jnp.int32, shape, 0)


def roll(x, shift):
    return pltpu.roll(x, shift % 128, 1)


def swap_blocks(a):
    lane = lanes()
    low = lane < 64
    even = (lane // 32) % 2 == 0
    p0 = jnp.where(low, a[0], roll(a[2], 64))
    p2 = jnp.where(low, roll(a[0], 64), a[2])
    p1 = jnp.where(low, a[1], roll(a[3], 64))
    p3 = jnp.where(low, roll(a[1], 64), a[3])
    return [
        jnp.where(even, p0, roll(p1, 32)),
        jnp.where(even, roll(p0, -32), p1),
        jnp.where(even, p2, roll(p3, 32)),
        jnp.where(even, roll(p2, -32), p3),
    ]


def to_table(faces):
    lane = lanes()
    ends = (lane >= J) & (lane < 32)
    more = (lane >= 32 + J) & (lane < 42 + J)
    first, second = [], []
    for half in range(2):
        part = [faces[8 * w : 8 * w + 8, 128 * half : 128 * half + 128] for w in range(V)]
        one = swap_blocks(part[0:4])
        two = swap_blocks(part[4:8])
        for b in range(4):
            kept = jnp.where(ends, roll(part[8], J - 32 * b), one[b])
            first.append(jnp.where(more, roll(part[8], 42 - 32 * b), kept))
            second.append(two[b])
    return jnp.concatenate(first, axis=0), jnp.concatenate(second, axis=0)


def from_table(first, second):
    lane = lanes()
    halves = []
    for half in range(2):
        one = [first[32 * half + 8 * b : 32 * half + 8 * b + 8] for b in range(4)]
        two = [second[32 * half + 8 * b : 32 * half + 8 * b + 8] for b in range(4)]
        last = jnp.zeros((8, 128), F32)
        for b in range(4):
            inside = lane - 32 * b
            last = jnp.where((inside >= 0) & (inside < 11), roll(one[b], 32 * b - J), last)
            last = jnp.where((inside >= 11) & (inside < J), roll(one[b], 32 * b - 42), last)
        halves.append(swap_blocks(one) + swap_blocks(two) + [last])
    return [jnp.concatenate([halves[0][w], halves[1][w]], axis=1) for w in range(V)]


def kernel(
    n_dom,
    n_sub,
    levels_hbm,
    source_hbm,
    send_hbm,
    fault_flux_hbm,
    fault_faces_hbm,
    dofs_hbm,
    stiff_hbm,
    proj_hbm,
    star_hbm,
    minus_hbm,
    plus_hbm,
    out_ref,
    levels_ref,
    source_ref,
    send_ref,
    fault_flux_ref,
    fault_faces_ref,
    dofs_ref,
    stiff_ref,
    proj_ref,
    star_ref,
    minus_ref,
    plus_ref,
    block_ref,
    pt_ref,
    x_ref,
    row_ref,
    wd_ref,
    wv_ref,
    pw_ref,
    pt3_ref,
    ptw_ref,
    cs_ref,
    cm_ref,
    cc_ref,
    flux_ref,
    msg_ref,
    recv_ref,
    in_sem,
    send_sem,
    recv_sem,
    across_sem,
):
    dom = lax.axis_index("dom")
    sub = lax.axis_index("sub")
    peers = []
    for delta, turn in FARTHEST_FIRST:
        peers.append((delta, lax.rem(dom + delta + n_dom, n_dom), lax.rem(sub + turn, n_sub)))

    odd = lax.rem(dom, 2)
    step = 2 * odd - 1
    partner = dom - step
    across = lax.rem(dom + step + n_dom, n_dom)
    behind = lax.rem(dom + 2 * step + n_dom, n_dom)
    subs = [lax.rem(sub + turn, n_sub) for turn in range(4)]
    barrier = pltpu.get_barrier_semaphore()

    def signal(to_dom, to_sub, which=barrier):
        pl.semaphore_signal(which, inc=1, device_id=(to_dom, to_sub), device_id_type=MESH)

    signal(behind, sub)
    for turn in (2, 1, 3):
        signal(dom, subs[turn])

    @pl.when(odd == 0)
    def _():
        for turn in (2, 1, 3):
            signal(behind, subs[turn])

    for turn in (2, 1, 3, 0):
        signal(partner, subs[turn])

    loads = [
        pltpu.make_async_copy(src, dst, in_sem.at[i])
        for i, (src, dst) in enumerate(
            (
                (stiff_hbm, stiff_ref),
                (star_hbm, star_ref),
                (dofs_hbm, dofs_ref),
                (proj_hbm, proj_ref),
                (minus_hbm, minus_ref),
                (plus_hbm, plus_ref),
                (levels_hbm, levels_ref),
                (source_hbm, source_ref),
                (send_hbm, send_ref),
                (fault_flux_hbm, fault_flux_ref),
                (fault_faces_hbm, fault_faces_ref),
            )
        )
    ]
    for load in loads:
        load.start()

    block_ref[...] = jnp.zeros(block_ref.shape, F32)
    pt_ref[...] = jnp.zeros(pt_ref.shape, F32)
    x_ref[...] = jnp.zeros(x_ref.shape, F32)
    row_ref[...] = jnp.zeros(row_ref.shape, F32)

    loads[0].wait()
    for d in range(3):
        block_ref[d, 0:M, 0:M] = stiff_ref[d]
        block_ref[d, 64 : 64 + M, 64 : 64 + M] = stiff_ref[d]
    for d in range(3):
        block = block_ref[d]
        wd_ref[:, 128 * d : 128 * d + 128] = rhs3(block.T)
        wv_ref[:, 128 * d : 128 * d + 128] = rhs3(block)

    def spread(make_row, groups, part_width, fill, coef_ref):
        width = 128 * coef_ref.shape[3] // 128
        k = lax.broadcasted_iota(jnp.int32, (128, width), 0) % 64
        lane = lax.broadcasted_iota(jnp.int32, (128, width), 1)
        group = lane // (2 * part_width)
        half = (lane // part_width) % 2
        hit = (k // E == group) & ((k % E) // 8 == half) & (lane % part_width < fill)
        repeat = hit.astype(F32).astype(BF16)
        keep = (lanes() % 8 == rows()).astype(F32)
        for v in range(V):
            row = make_row(v)
            high = row.astype(BF16).astype(F32)
            row_ref[v, 0:V, 0 : groups * E] = high
            row_ref[v, 0:V, 64 : 64 + groups * E] = row - high
        for v in range(V):
            left = jnp.concatenate(
                [jnp.broadcast_to(row_ref[v, w : w + 1, :], (8, 128)) * keep for w in range(V)],
                axis=0,
            ).astype(BF16)
            coef_ref[v] = dot(left, repeat).reshape(V, 8, width)

    loads[1].wait()
    spread(
        lambda v: jnp.concatenate([star_ref[v, :, d, :] for d in range(3)], axis=1),
        3,
        64,
        M,
        cs_ref,
    )

    loads[2].wait()
    for v in range(V):
        x_ref[8 * v : 8 * v + 8, 0:M] = dofs_ref[v, 0:8, :]
        x_ref[8 * v : 8 * v + 8, 64 : 64 + M] = dofs_ref[v, 8:16, :]

    def contract(coef_ref, field, v):
        return (coef_ref[v] * field).sum(axis=0)

    def with_star(weights_ref, left):
        return star_sum(dot(left, weights_ref[...]))

    def star_sum(field):
        field = field.reshape(V, 8, 384)
        result = []
        for v in range(V):
            total = contract(cs_ref, field, v)
            result.append(total[:, 0:128] + total[:, 128:256] + total[:, 256:384])
        return jnp.concatenate(result, axis=0)

    def series(start, want_second, opening=None):
        current = start
        first = FIRST[0] * current
        second = SECOND[0] * current if want_second else None
        for k in range(1, ORDER):
            if k == 1 and opening is not None:
                current = star_sum(opening)
            else:
                current = with_star(wd_ref, lhs3(current))
            first = first + FIRST[k] * current
            if want_second:
                second = second + SECOND[k] * current
        return first, second

    loads[3].wait()
    for f in range(4):
        for half in range(2):
            at = 64 * f + 32 * half
            pt_ref[at : at + J, 64 * half : 64 * half + M] = proj_ref[:, f, :]
    pt = pt_ref[...]
    pw_ref[...] = rhs3(pt.T)
    pt3_ref[...] = rhs3(pt)

    for i in (6, 7, 8):
        loads[i].wait()
    row = rows((8, 256))
    lane = lanes((8, 256))
    wanted = jnp.full((8, 256), -1, jnp.int32)
    for s in range(4):
        wanted = jnp.where(row % 4 == s, send_ref[s], wanted)
    pick_send = ((lane % 64 == wanted) & (lane // 128 == row // 4)).astype(F32).astype(BF16)

    local_rows, remote_rows = [], []
    row = rows()
    lane = lanes()
    lane2 = lanes((8, 192)) % 96
    for f in range(4):
        for half in range(2):
            wanted = jnp.full((8, 128), -1, jnp.int32)
            for i in range(8):
                wanted = jnp.where(row == i, source_ref[f, 8 * half + i], wanted)
            local_rows.append((lane % 64 == wanted).astype(F32))
            far = wanted - 64
            code = jnp.where(far >= 0, (far // 4) * 8 + far % 4, -8)
            code = jnp.concatenate([code, code[:, 0:64]], axis=1)
            remote_rows.append((code, lane2))
    pick_local = jnp.concatenate(local_rows, axis=0).astype(BF16)
    pick_remote = jnp.concatenate(
        [(at == code + 4 * q).astype(F32) for q in range(2) for code, at in remote_rows], axis=0
    ).astype(BF16)

    fine = jnp.zeros((8, 128), jnp.int32)
    for e in range(E):
        here = (row == e % 8) & (lane // 64 == e // 8)
        fine = jnp.where(here & (levels_ref[e] == 0), 1, fine)
    fine = jnp.concatenate([fine] * V, axis=0) == 1

    dofs = x_ref[...]
    first_half, second_half = series(dofs, True)
    pl.semaphore_wait(barrier, 11 - 3 * odd)
    signal(partner, sub, across_sem)

    def make_message(turn, table):
        stacked = jnp.concatenate([stack2(table[0]), stack2(table[1])], axis=0)
        message = dot(pick_send, stacked)
        msg_ref[turn] = message
        recv_ref[turn, 4 + sub] = message

    def message_to(turn, slot, to_dom, to_sub, arrival):
        return pltpu.make_async_remote_copy(
            src_ref=msg_ref.at[turn],
            dst_ref=recv_ref.at[turn, slot],
            send_sem=send_sem.at[turn],
            recv_sem=arrival,
            device_id=(to_dom, to_sub),
            device_id_type=MESH,
        )

    def several(turn, count, arrival):
        some = recv_ref.at[turn, pl.ds(0, count)]
        return pltpu.make_async_remote_copy(
            src_ref=some,
            dst_ref=some,
            send_sem=send_sem.at[turn],
            recv_sem=arrival,
            device_id=(dom, subs[1]),
            device_id_type=MESH,
        )

    def start_first():
        @pl.when(odd == 1)
        def _():
            pl.semaphore_wait(across_sem, 1)
            for turn in (2, 1, 3, 0):
                message_to(0, sub, across, subs[turn], recv_sem.at[0]).start()

        for turn in (2, 1, 3):
            message_to(0, 4 + sub, dom, subs[turn], recv_sem.at[2]).start()
        for turn in (2, 1, 3, 0):
            message_to(0, 8 * odd + sub, partner, subs[turn], recv_sem.at[0]).start()

    def finish_first():
        several(0, 3, recv_sem.at[2]).wait_recv()

        @pl.when(odd == 0)
        def _():
            pl.semaphore_wait(across_sem, 1)
            pltpu.make_async_remote_copy(
                src_ref=recv_ref.at[0, pl.ds(4, 4)],
                dst_ref=recv_ref.at[0, pl.ds(8, 4)],
                send_sem=send_sem.at[0],
                recv_sem=recv_sem.at[0],
                device_id=(across, sub),
                device_id_type=MESH,
            ).start()

        several(0, 8, recv_sem.at[0]).wait_recv()

    def start_second():
        for delta, to_dom, to_sub in peers:
            message_to(1, 4 * (1 - delta) + sub, to_dom, to_sub, recv_sem.at[1]).start()

    def local_part(table):
        return dot(pick_local, jnp.concatenate([stack2(table[0]), stack2(table[1])], axis=1))

    def beside_faces(turn, near):
        arrived = stack2(recv_ref[turn].reshape(8 * SLOTS, 128))
        faces = from_table(
            near[:, 0:128] + dot(pick_remote[0:64], arrived),
            near[:, 128:256] + dot(pick_remote[64:128], arrived),
        )
        return jnp.concatenate(faces, axis=0).reshape(V, 8, 256)

    left = lhs3(first_half)
    faces = dot(left, pw_ref[...])
    table = to_table(faces)
    make_message(0, table)
    start_first()

    loads[4].wait()
    spread(
        lambda v: jnp.concatenate([minus_ref[v, :, f, :] for f in range(4)], axis=1),
        4,
        32,
        J,
        cm_ref,
    )
    for i in (5, 9, 10):
        loads[i].wait()
    on_fault = jnp.concatenate([fault_faces_ref[f : f + 1, :] for f in range(4)], axis=1) == 1

    def coupling_row(v):
        plus = jnp.concatenate([plus_ref[v, :, f, :] for f in range(4)], axis=1)
        w_at = rows((V, 4 * E))
        friction = jnp.zeros((V, 4 * E), F32)
        for w in range(V):
            friction = jnp.where(w_at == w, fault_flux_ref[v, w], friction)
        return jnp.where(jnp.broadcast_to(on_fault, (V, 4 * E)), friction, plus)

    spread(coupling_row, 4, 32, J, cc_ref)

    def own_side(left, faces):
        volume = with_star(wv_ref, left)
        field = faces.reshape(V, 8, 256)
        for v in range(V):
            flux_ref[8 * v : 8 * v + 8, :] = contract(cm_ref, field, v)
        return volume

    def fluxes(turn, near):
        field = beside_faces(turn, near)
        total = jnp.concatenate([contract(cc_ref, field, v) for v in range(V)], axis=0)
        hi, lo = split(total + flux_ref[...])
        return jnp.concatenate([hi, lo], axis=1), hi

    near = local_part(table)
    base = dofs + own_side(left, faces)
    base_slopes = dot(lhs3(base), wd_ref[...])
    ptw_ref[...] = rhs3(dot(lhs3(pt), wd_ref[...]))
    finish_first()
    both, hi = fluxes(0, near)
    opening = base_slopes - dot(both, ptw_ref[0:512, :]) - dot(hi, ptw_ref[512:768, :])
    moved = base - dot(both, pt3_ref[0:512, :]) - dot(hi, pt3_ref[512:768, :])

    again, _ = series(moved, False, opening)
    carried = jnp.where(fine, again, second_half)
    left = lhs3(carried)
    faces = dot(left, pw_ref[...])
    table = to_table(faces)
    make_message(1, table)
    start_second()
    near = local_part(table)
    base = moved + own_side(left, faces)
    for turn in range(2):
        several(turn, len(peers), recv_sem.at[turn]).wait_send()
    several(1, len(peers), recv_sem.at[1]).wait_recv()
    both, hi = fluxes(1, near)
    after = base - dot(both, pt3_ref[0:512, :]) - dot(hi, pt3_ref[512:768, :])
    for v in range(V):
        out_ref[v, 0:8, :] = after[8 * v : 8 * v + 8, 0:M]
        out_ref[v, 8:16, :] = after[8 * v : 8 * v + 8, 64 : 64 + M]


def per_device(
    n_dom,
    n_sub,
    dofs,
    stiffness,
    projection,
    star,
    flux_minus,
    flux_plus,
    fault_flux,
    fault_faces,
    levels,
    face_source,
    send_source,
):
    vmem = pl.BlockSpec(memory_space=pltpu.VMEM)
    hbm = pl.BlockSpec(memory_space=pltpu.HBM)
    result = pl.pallas_call(
        functools.partial(kernel, n_dom, n_sub),
        out_shape=pltpu.VMEM((V, E, M), F32),
        in_specs=[hbm] * 11,
        out_specs=vmem,
        scratch_shapes=[
            pltpu.SMEM((E,), jnp.int32),
            pltpu.SMEM((4, E), jnp.int32),
            pltpu.SMEM((4,), jnp.int32),
            pltpu.SMEM((V, V), F32),
            pltpu.VMEM((4, E), jnp.int32),
            pltpu.VMEM((V, E, M), F32),
            pltpu.VMEM((3, M, M), F32),
            pltpu.VMEM((J, 4, M), F32),
            pltpu.VMEM((V, V, 3, E), F32),
            pltpu.VMEM((V, V, 4, E), F32),
            pltpu.VMEM((V, V, 4, E), F32),
            pltpu.VMEM((3, 128, 128), F32),
            pltpu.VMEM((256, 128), F32),
            pltpu.VMEM((72, 128), F32),
            pltpu.VMEM((V, 16, 128), F32),
            pltpu.VMEM((384, 384), BF16),
            pltpu.VMEM((384, 384), BF16),
            pltpu.VMEM((384, 256), BF16),
            pltpu.VMEM((768, 128), BF16),
            pltpu.VMEM((768, 384), BF16),
            pltpu.VMEM((V, V, 8, 384), F32),
            pltpu.VMEM((V, V, 8, 256), F32),
            pltpu.VMEM((V, V, 8, 256), F32),
            pltpu.VMEM((72, 256), F32),
            pltpu.VMEM((2, 8, 128), F32),
            pltpu.VMEM((2, SLOTS, 8, 128), F32),
            pltpu.SemaphoreType.DMA((11,)),
            pltpu.SemaphoreType.DMA((2,)),
            pltpu.SemaphoreType.DMA((3,)),
            pltpu.SemaphoreType.REGULAR,
        ],
        compiler_params=pltpu.CompilerParams(
            collective_id=0, has_side_effects=True, vmem_limit_bytes=VMEM_LIMIT
        ),
    )(
        *(
            pltpu.with_memory_space_constraint(x, pltpu.HBM)
            for x in (
        levels,
        face_source,
        send_source,
        fault_flux,
        fault_faces,
        jnp.transpose(dofs, (0, 2, 1)),
        stiffness,
        jnp.transpose(projection, (1, 0, 2)),
        jnp.transpose(star, (1, 2, 0, 3)),
        jnp.transpose(flux_minus, (1, 2, 0, 3)),
        jnp.transpose(flux_plus, (1, 2, 0, 3)),
                )
        )
    )
    return jnp.transpose(result, (0, 2, 1))


def solution(mesh):
    return jax.shard_map(
        functools.partial(per_device, mesh.shape["dom"], mesh.shape["sub"]),
        mesh=mesh,
        in_specs=(
            P(None, None, ("dom", "sub")),
            P(),
            P(),
            P(None, None, None, ("dom", "sub")),
            P(None, None, None, ("dom", "sub")),
            P(None, None, None, ("dom", "sub")),
            P(),
            P(None, ("dom", "sub")),
            P(("dom", "sub")),
            P(None, ("dom", "sub")),
            P(("dom", "sub")),
        ),
        out_specs=P(None, None, ("dom", "sub")),
        check_vma=False,
    )
```

```python
import functools
import math

import jax
import jax.numpy as jnp
from jax import lax
from jax.experimental import pallas as pl
from jax.experimental.pallas import tpu as pltpu
from jax.sharding import PartitionSpec as P

ORDER = 6
TAU = 0.75
V = 9
M = 56
J = 21
E = 16
SLOTS = 12
VMEM_LIMIT = 24 * 2**20
FARTHEST_FIRST = (
    (-1, 2),
    (1, 2),
    (-1, 1),
    (1, 1),
    (-1, 3),
    (1, 3),
    (0, 2),
    (-1, 0),
    (1, 0),
    (0, 1),
    (0, 3),
)
MESH = pl.DeviceIdType.MESH
F32 = jnp.float32
BF16 = jnp.bfloat16


def taylor_weights(start_time, stop_time):
    return [
        (stop_time ** (k + 1) - start_time ** (k + 1)) / math.factorial(k + 1)
        for k in range(ORDER)
    ]


FIRST = taylor_weights(0.0, TAU)
SECOND = taylor_weights(TAU, 2.0 * TAU)


def split(x):
    hi = x.astype(BF16)
    return hi, (x - hi.astype(F32)).astype(BF16)


def lhs3(x):
    hi, lo = split(x)
    return jnp.concatenate([hi, lo, hi], axis=1)


def rhs3(x):
    hi, lo = split(x)
    return jnp.concatenate([hi, hi, lo], axis=0)


def stack2(x):
    hi, lo = split(x)
    return jnp.concatenate([hi, lo], axis=0)


def dot(a, b):
    return jnp.dot(a, b, preferred_element_type=F32)


def lanes(shape=(8, 128)):
    return lax.broadcasted_iota(jnp.int32, shape, 1)


def rows(shape=(8, 128)):
    return lax.broadcasted_iota(jnp.int32, shape, 0)


def roll(x, shift):
    return pltpu.roll(x, shift % 128, 1)


def swap_blocks(a):
    lane = lanes()
    low = lane < 64
    even = (lane // 32) % 2 == 0
    p0 = jnp.where(low, a[0], roll(a[2], 64))
    p2 = jnp.where(low, roll(a[0], 64), a[2])
    p1 = jnp.where(low, a[1], roll(a[3], 64))
    p3 = jnp.where(low, roll(a[1], 64), a[3])
    return [
        jnp.where(even, p0, roll(p1, 32)),
        jnp.where(even, roll(p0, -32), p1),
        jnp.where(even, p2, roll(p3, 32)),
        jnp.where(even, roll(p2, -32), p3),
    ]


def to_table(faces):
    lane = lanes()
    ends = (lane >= J) & (lane < 32)
    more = (lane >= 32 + J) & (lane < 42 + J)
    first, second = [], []
    for half in range(2):
        part = [faces[8 * w : 8 * w + 8, 128 * half : 128 * half + 128] for w in range(V)]
        one = swap_blocks(part[0:4])
        two = swap_blocks(part[4:8])
        for b in range(4):
            kept = jnp.where(ends, roll(part[8], J - 32 * b), one[b])
            first.append(jnp.where(more, roll(part[8], 42 - 32 * b), kept))
            second.append(two[b])
    return jnp.concatenate(first, axis=0), jnp.concatenate(second, axis=0)


def from_table(first, second):
    lane = lanes()
    halves = []
    for half in range(2):
        one = [first[32 * half + 8 * b : 32 * half + 8 * b + 8] for b in range(4)]
        two = [second[32 * half + 8 * b : 32 * half + 8 * b + 8] for b in range(4)]
        last = jnp.zeros((8, 128), F32)
        for b in range(4):
            inside = lane - 32 * b
            last = jnp.where((inside >= 0) & (inside < 11), roll(one[b], 32 * b - J), last)
            last = jnp.where((inside >= 11) & (inside < J), roll(one[b], 32 * b - 42), last)
        halves.append(swap_blocks(one) + swap_blocks(two) + [last])
    return [jnp.concatenate([halves[0][w], halves[1][w]], axis=1) for w in range(V)]


def kernel(
    n_dom,
    n_sub,
    levels_hbm,
    source_hbm,
    send_hbm,
    fault_flux_hbm,
    fault_faces_hbm,
    dofs_hbm,
    stiff_hbm,
    proj_hbm,
    star_hbm,
    minus_hbm,
    plus_hbm,
    out_ref,
    levels_ref,
    source_ref,
    send_ref,
    fault_flux_ref,
    fault_faces_ref,
    dofs_ref,
    stiff_ref,
    proj_ref,
    star_ref,
    minus_ref,
    plus_ref,
    block_ref,
    pt_ref,
    x_ref,
    row_ref,
    wd_ref,
    wv_ref,
    pw_ref,
    pt3_ref,
    ptw_ref,
    cs_ref,
    cm_ref,
    cc_ref,
    flux_ref,
    msg_ref,
    recv_ref,
    in_sem,
    send_sem,
    recv_sem,
    across_sem,
):
    dom = lax.axis_index("dom")
    sub = lax.axis_index("sub")
    peers = []
    for delta, turn in FARTHEST_FIRST:
        peers.append((delta, lax.rem(dom + delta + n_dom, n_dom), lax.rem(sub + turn, n_sub)))

    def strided(src, dst, count, at):
        return [
            pltpu.make_async_copy(
                src.at[:, w], dst.at[:, pl.ds(4 * w, count), :], in_sem.at[at]
            )
            for w in range(V)
        ]

    star_loads = strided(star_hbm, star_ref, 3, 8)
    minus_loads = strided(minus_hbm, minus_ref, 4, 9)
    plus_loads = strided(plus_hbm, plus_ref, 4, 10)
    loads = [
        pltpu.make_async_copy(src, dst, in_sem.at[i])
        for i, (src, dst) in enumerate(
            (
                (stiff_hbm, stiff_ref),
                (dofs_hbm, dofs_ref),
                (proj_hbm, proj_ref),
                (send_hbm, send_ref),
                (levels_hbm, levels_ref),
                (source_hbm, source_ref),
                (fault_flux_hbm, fault_flux_ref),
                (fault_faces_hbm, fault_faces_ref),
            )
        )
    ]
    for load in loads[0:1] + star_loads + loads[1:] + minus_loads + plus_loads:
        load.start()

    def wait_whole(src, at):
        pltpu.make_async_copy(src, src, in_sem.at[at]).wait()

    def wait(*which):
        for load in which:
            load.wait()

    odd = lax.rem(dom, 2)
    step = 2 * odd - 1
    partner = dom - step
    across = lax.rem(dom + step + n_dom, n_dom)
    behind = lax.rem(dom + 2 * step + n_dom, n_dom)
    subs = [lax.rem(sub + turn, n_sub) for turn in range(4)]
    barrier = pltpu.get_barrier_semaphore()

    def signal(to_dom, to_sub, which=barrier):
        pl.semaphore_signal(which, inc=1, device_id=(to_dom, to_sub), device_id_type=MESH)

    signal(behind, sub)
    for turn in (2, 1, 3):
        signal(dom, subs[turn])

    @pl.when(odd == 0)
    def _():
        for turn in (2, 1, 3):
            signal(behind, subs[turn])

    for turn in (2, 1, 3, 0):
        signal(partner, subs[turn])

    block_ref[...] = jnp.zeros(block_ref.shape, F32)
    pt_ref[...] = jnp.zeros(pt_ref.shape, F32)
    x_ref[...] = jnp.zeros(x_ref.shape, F32)
    row_ref[...] = jnp.zeros(row_ref.shape, F32)

    wait(loads[0])
    for d in range(3):
        block_ref[d, 0:M, 0:M] = stiff_ref[d]
        block_ref[d, 64 : 64 + M, 64 : 64 + M] = stiff_ref[d]
    for d in range(3):
        block = block_ref[d]
        wd_ref[:, 128 * d : 128 * d + 128] = rhs3(block.T)
        wv_ref[:, 128 * d : 128 * d + 128] = rhs3(block)

    wait(loads[2])
    for f in range(4):
        for half in range(2):
            at = 64 * f + 32 * half
            pt_ref[at : at + J, 64 * half : 64 * half + M] = proj_ref[:, f, :]
    pt = pt_ref[...]
    pw_ref[...] = rhs3(pt.T)

    wait(loads[3])
    row = rows((8, 256))
    lane = lanes((8, 256))
    wanted = jnp.full((8, 256), -1, jnp.int32)
    for s in range(4):
        wanted = jnp.where(row % 4 == s, send_ref[s], wanted)
    pick_send = ((lane % 64 == wanted) & (lane // 128 == row // 4)).astype(F32).astype(BF16)

    def spread(make_row, groups, part_width, fill, coef_ref):
        width = 128 * coef_ref.shape[3] // 128
        k = lax.broadcasted_iota(jnp.int32, (128, width), 0) % 64
        lane = lax.broadcasted_iota(jnp.int32, (128, width), 1)
        group = lane // (2 * part_width)
        half = (lane // part_width) % 2
        hit = (k // E == group) & ((k % E) // 8 == half) & (lane % part_width < fill)
        repeat = hit.astype(F32).astype(BF16)
        keep = (lanes() % 8 == rows()).astype(F32)
        for v in range(V):
            row = make_row(v)
            high = row.astype(BF16).astype(F32)
            row_ref[v, 0:V, 0 : groups * E] = high
            row_ref[v, 0:V, 64 : 64 + groups * E] = row - high
        for v in range(V):
            left = jnp.concatenate(
                [jnp.broadcast_to(row_ref[v, w : w + 1, :], (8, 128)) * keep for w in range(V)],
                axis=0,
            ).astype(BF16)
            coef_ref[v] = dot(left, repeat).reshape(V, 8, width)

    wait_whole(star_hbm, 8)
    spread(
        lambda v: jnp.concatenate([star_ref[v, pl.ds(d, V, stride=4), :] for d in range(3)], axis=1),
        3,
        64,
        M,
        cs_ref,
    )

    wait(loads[1])
    for v in range(V):
        x_ref[8 * v : 8 * v + 8, 0:M] = dofs_ref[v, 0:8, :]
        x_ref[8 * v : 8 * v + 8, 64 : 64 + M] = dofs_ref[v, 8:16, :]

    def contract(coef_ref, field, v):
        return (coef_ref[v] * field).sum(axis=0)

    def with_star(weights_ref, left):
        return star_sum(dot(left, weights_ref[...]))

    def star_sum(field):
        field = field.reshape(V, 8, 384)
        result = []
        for v in range(V):
            total = contract(cs_ref, field, v)
            result.append(total[:, 0:128] + total[:, 128:256] + total[:, 256:384])
        return jnp.concatenate(result, axis=0)

    def series(start, want_second, opening=None):
        current = start
        first = FIRST[0] * current
        second = SECOND[0] * current if want_second else None
        for k in range(1, ORDER):
            if k == 1 and opening is not None:
                current = star_sum(opening)
            else:
                current = with_star(wd_ref, lhs3(current))
            first = first + FIRST[k] * current
            if want_second:
                second = second + SECOND[k] * current
        return first, second

    dofs = x_ref[...]
    first_half, second_half = series(dofs, True)
    pl.semaphore_wait(barrier, 11 - 3 * odd)
    signal(partner, sub, across_sem)

    def make_message(turn, table):
        stacked = jnp.concatenate([stack2(table[0]), stack2(table[1])], axis=0)
        message = dot(pick_send, stacked)
        msg_ref[turn] = message
        recv_ref[turn, 4 + sub] = message

    def message_to(turn, slot, to_dom, to_sub, arrival):
        return pltpu.make_async_remote_copy(
            src_ref=msg_ref.at[turn],
            dst_ref=recv_ref.at[turn, slot],
            send_sem=send_sem.at[turn],
            recv_sem=arrival,
            device_id=(to_dom, to_sub),
            device_id_type=MESH,
        )

    def several(turn, count, arrival):
        some = recv_ref.at[turn, pl.ds(0, count)]
        return pltpu.make_async_remote_copy(
            src_ref=some,
            dst_ref=some,
            send_sem=send_sem.at[turn],
            recv_sem=arrival,
            device_id=(dom, subs[1]),
            device_id_type=MESH,
        )

    def start_first():
        @pl.when(odd == 1)
        def _():
            pl.semaphore_wait(across_sem, 1)
            for turn in (2, 1, 3, 0):
                message_to(0, sub, across, subs[turn], recv_sem.at[0]).start()

        for turn in (2, 1, 3):
            message_to(0, 4 + sub, dom, subs[turn], recv_sem.at[2]).start()
        for turn in (2, 1, 3, 0):
            message_to(0, 8 * odd + sub, partner, subs[turn], recv_sem.at[0]).start()

    def finish_first():
        several(0, 3, recv_sem.at[2]).wait_recv()

        @pl.when(odd == 0)
        def _():
            pl.semaphore_wait(across_sem, 1)
            pltpu.make_async_remote_copy(
                src_ref=recv_ref.at[0, pl.ds(4, 4)],
                dst_ref=recv_ref.at[0, pl.ds(8, 4)],
                send_sem=send_sem.at[0],
                recv_sem=recv_sem.at[0],
                device_id=(across, sub),
                device_id_type=MESH,
            ).start()

        several(0, 8, recv_sem.at[0]).wait_recv()

    def start_second():
        for delta, to_dom, to_sub in peers:
            message_to(1, 4 * (1 - delta) + sub, to_dom, to_sub, recv_sem.at[1]).start()

    def local_part(table):
        return dot(pick_local, jnp.concatenate([stack2(table[0]), stack2(table[1])], axis=1))

    def beside_faces(turn, near):
        arrived = stack2(recv_ref[turn].reshape(8 * SLOTS, 128))
        faces = from_table(
            near[:, 0:128] + dot(pick_remote[0:64], arrived),
            near[:, 128:256] + dot(pick_remote[64:128], arrived),
        )
        return jnp.concatenate(faces, axis=0).reshape(V, 8, 256)

    left = lhs3(first_half)
    faces = dot(left, pw_ref[...])
    table = to_table(faces)
    make_message(0, table)
    start_first()

    pt3_ref[...] = rhs3(pt)
    wait(*loads[4:6])
    local_rows, remote_rows = [], []
    row = rows()
    lane = lanes()
    lane2 = lanes((8, 192)) % 96
    for f in range(4):
        for half in range(2):
            wanted = jnp.full((8, 128), -1, jnp.int32)
            for i in range(8):
                wanted = jnp.where(row == i, source_ref[f, 8 * half + i], wanted)
            local_rows.append((lane % 64 == wanted).astype(F32))
            far = wanted - 64
            code = jnp.where(far >= 0, (far // 4) * 8 + far % 4, -8)
            code = jnp.concatenate([code, code[:, 0:64]], axis=1)
            remote_rows.append((code, lane2))
    pick_local = jnp.concatenate(local_rows, axis=0).astype(BF16)
    pick_remote = jnp.concatenate(
        [(at == code + 4 * q).astype(F32) for q in range(2) for code, at in remote_rows], axis=0
    ).astype(BF16)

    fine = jnp.zeros((8, 128), jnp.int32)
    for e in range(E):
        here = (row == e % 8) & (lane // 64 == e // 8)
        fine = jnp.where(here & (levels_ref[e] == 0), 1, fine)
    fine = jnp.concatenate([fine] * V, axis=0) == 1

    wait_whole(minus_hbm, 9)
    spread(
        lambda v: jnp.concatenate([minus_ref[v, pl.ds(f, V, stride=4), :] for f in range(4)], axis=1),
        4,
        32,
        J,
        cm_ref,
    )
    wait_whole(plus_hbm, 10)
    wait(*loads[6:8])
    on_fault = jnp.concatenate([fault_faces_ref[f : f + 1, :] for f in range(4)], axis=1) == 1

    def coupling_row(v):
        plus = jnp.concatenate([plus_ref[v, pl.ds(f, V, stride=4), :] for f in range(4)], axis=1)
        w_at = rows((V, 4 * E))
        friction = jnp.zeros((V, 4 * E), F32)
        for w in range(V):
            friction = jnp.where(w_at == w, fault_flux_ref[v, w], friction)
        return jnp.where(jnp.broadcast_to(on_fault, (V, 4 * E)), friction, plus)

    spread(coupling_row, 4, 32, J, cc_ref)

    def own_side(left, faces):
        volume = with_star(wv_ref, left)
        field = faces.reshape(V, 8, 256)
        for v in range(V):
            flux_ref[8 * v : 8 * v + 8, :] = contract(cm_ref, field, v)
        return volume

    def fluxes(turn, near):
        field = beside_faces(turn, near)
        total = jnp.concatenate([contract(cc_ref, field, v) for v in range(V)], axis=0)
        hi, lo = split(total + flux_ref[...])
        return jnp.concatenate([hi, lo], axis=1), hi

    near = local_part(table)
    base = dofs + own_side(left, faces)
    base_slopes = dot(lhs3(base), wd_ref[...])
    ptw_ref[...] = rhs3(dot(lhs3(pt), wd_ref[...]))
    finish_first()
    both, hi = fluxes(0, near)
    opening = base_slopes - dot(both, ptw_ref[0:512, :]) - dot(hi, ptw_ref[512:768, :])
    moved = base - dot(both, pt3_ref[0:512, :]) - dot(hi, pt3_ref[512:768, :])

    again, _ = series(moved, False, opening)
    carried = jnp.where(fine, again, second_half)
    left = lhs3(carried)
    faces = dot(left, pw_ref[...])
    table = to_table(faces)
    make_message(1, table)
    start_second()
    near = local_part(table)
    base = moved + own_side(left, faces)
    for turn in range(2):
        several(turn, len(peers), recv_sem.at[turn]).wait_send()
    several(1, len(peers), recv_sem.at[1]).wait_recv()
    both, hi = fluxes(1, near)
    after = base - dot(both, pt3_ref[0:512, :]) - dot(hi, pt3_ref[512:768, :])
    for v in range(V):
        out_ref[v, 0:8, :] = after[8 * v : 8 * v + 8, 0:M]
        out_ref[v, 8:16, :] = after[8 * v : 8 * v + 8, 64 : 64 + M]


def per_device(
    n_dom,
    n_sub,
    dofs,
    stiffness,
    projection,
    star,
    flux_minus,
    flux_plus,
    fault_flux,
    fault_faces,
    levels,
    face_source,
    send_source,
):
    vmem = pl.BlockSpec(memory_space=pltpu.VMEM)
    hbm = pl.BlockSpec(memory_space=pltpu.HBM)
    result = pl.pallas_call(
        functools.partial(kernel, n_dom, n_sub),
        out_shape=pltpu.VMEM((V, E, M), F32),
        in_specs=[hbm] * 11,
        out_specs=vmem,
        scratch_shapes=[
            pltpu.SMEM((E,), jnp.int32),
            pltpu.SMEM((4, E), jnp.int32),
            pltpu.SMEM((4,), jnp.int32),
            pltpu.SMEM((V, V), F32),
            pltpu.VMEM((4, E), jnp.int32),
            pltpu.VMEM((V, E, M), F32),
            pltpu.VMEM((3, M, M), F32),
            pltpu.VMEM((J, 4, M), F32),
            pltpu.VMEM((V, 4 * V, E), F32),
            pltpu.VMEM((V, 4 * V, E), F32),
            pltpu.VMEM((V, 4 * V, E), F32),
            pltpu.VMEM((3, 128, 128), F32),
            pltpu.VMEM((256, 128), F32),
            pltpu.VMEM((72, 128), F32),
            pltpu.VMEM((V, 16, 128), F32),
            pltpu.VMEM((384, 384), BF16),
            pltpu.VMEM((384, 384), BF16),
            pltpu.VMEM((384, 256), BF16),
            pltpu.VMEM((768, 128), BF16),
            pltpu.VMEM((768, 384), BF16),
            pltpu.VMEM((V, V, 8, 384), F32),
            pltpu.VMEM((V, V, 8, 256), F32),
            pltpu.VMEM((V, V, 8, 256), F32),
            pltpu.VMEM((72, 256), F32),
            pltpu.VMEM((2, 8, 128), F32),
            pltpu.VMEM((2, SLOTS, 8, 128), F32),
            pltpu.SemaphoreType.DMA((11,)),
            pltpu.SemaphoreType.DMA((2,)),
            pltpu.SemaphoreType.DMA((3,)),
            pltpu.SemaphoreType.REGULAR,
        ],
        compiler_params=pltpu.CompilerParams(
            collective_id=0, has_side_effects=True, vmem_limit_bytes=VMEM_LIMIT
        ),
    )(
        *(
            pltpu.with_memory_space_constraint(x, pltpu.HBM)
            for x in (
        levels,
        face_source,
        send_source,
        fault_flux,
        fault_faces,
        jnp.transpose(dofs, (0, 2, 1)),
        stiffness,
        jnp.transpose(projection, (1, 0, 2)),
        jnp.transpose(star, (1, 2, 0, 3)),
        jnp.transpose(flux_minus, (1, 2, 0, 3)),
        jnp.transpose(flux_plus, (1, 2, 0, 3)),
                )
        )
    )
    return jnp.transpose(result, (0, 2, 1))


def solution(mesh):
    return jax.shard_map(
        functools.partial(per_device, mesh.shape["dom"], mesh.shape["sub"]),
        mesh=mesh,
        in_specs=(
            P(None, None, ("dom", "sub")),
            P(),
            P(),
            P(None, None, None, ("dom", "sub")),
            P(None, None, None, ("dom", "sub")),
            P(None, None, None, ("dom", "sub")),
            P(),
            P(None, ("dom", "sub")),
            P(("dom", "sub")),
            P(None, ("dom", "sub")),
            P(("dom", "sub")),
        ),
        out_specs=P(None, None, ("dom", "sub")),
        check_vma=False,
    )
```

```python
import functools
import math

import jax
import jax.numpy as jnp
from jax import lax
from jax.experimental import pallas as pl
from jax.experimental.pallas import tpu as pltpu
from jax.sharding import PartitionSpec as P

ORDER = 6
TAU = 0.75
V = 9
M = 56
J = 21
E = 16
SLOTS = 12
VMEM_LIMIT = 24 * 2**20
FARTHEST_FIRST = (
    (-1, 2),
    (1, 2),
    (-1, 1),
    (1, 1),
    (-1, 3),
    (1, 3),
    (0, 2),
    (-1, 0),
    (1, 0),
    (0, 1),
    (0, 3),
)
MESH = pl.DeviceIdType.MESH
F32 = jnp.float32
BF16 = jnp.bfloat16


def taylor_weights(start_time, stop_time):
    return [
        (stop_time ** (k + 1) - start_time ** (k + 1)) / math.factorial(k + 1)
        for k in range(ORDER)
    ]


FIRST = taylor_weights(0.0, TAU)
SECOND = taylor_weights(TAU, 2.0 * TAU)


def split(x):
    hi = x.astype(BF16)
    return hi, (x - hi.astype(F32)).astype(BF16)


def lhs3(x):
    hi, lo = split(x)
    return jnp.concatenate([hi, lo, hi], axis=1)


def rhs3(x):
    hi, lo = split(x)
    return jnp.concatenate([hi, hi, lo], axis=0)


def stack2(x):
    hi, lo = split(x)
    return jnp.concatenate([hi, lo], axis=0)


def dot(a, b):
    return jnp.dot(a, b, preferred_element_type=F32)


def lanes(shape=(8, 128)):
    return lax.broadcasted_iota(jnp.int32, shape, 1)


def rows(shape=(8, 128)):
    return lax.broadcasted_iota(jnp.int32, shape, 0)


def roll(x, shift):
    return pltpu.roll(x, shift % 128, 1)


def swap_blocks(a):
    lane = lanes()
    low = lane < 64
    even = (lane // 32) % 2 == 0
    p0 = jnp.where(low, a[0], roll(a[2], 64))
    p2 = jnp.where(low, roll(a[0], 64), a[2])
    p1 = jnp.where(low, a[1], roll(a[3], 64))
    p3 = jnp.where(low, roll(a[1], 64), a[3])
    return [
        jnp.where(even, p0, roll(p1, 32)),
        jnp.where(even, roll(p0, -32), p1),
        jnp.where(even, p2, roll(p3, 32)),
        jnp.where(even, roll(p2, -32), p3),
    ]


def to_table(faces):
    lane = lanes()
    ends = (lane >= J) & (lane < 32)
    more = (lane >= 32 + J) & (lane < 42 + J)
    first, second = [], []
    for half in range(2):
        part = [faces[8 * w : 8 * w + 8, 128 * half : 128 * half + 128] for w in range(V)]
        one = swap_blocks(part[0:4])
        two = swap_blocks(part[4:8])
        for b in range(4):
            kept = jnp.where(ends, roll(part[8], J - 32 * b), one[b])
            first.append(jnp.where(more, roll(part[8], 42 - 32 * b), kept))
            second.append(two[b])
    return jnp.concatenate(first, axis=0), jnp.concatenate(second, axis=0)


def from_table(first, second):
    lane = lanes()
    halves = []
    for half in range(2):
        one = [first[32 * half + 8 * b : 32 * half + 8 * b + 8] for b in range(4)]
        two = [second[32 * half + 8 * b : 32 * half + 8 * b + 8] for b in range(4)]
        last = jnp.zeros((8, 128), F32)
        for b in range(4):
            inside = lane - 32 * b
            last = jnp.where((inside >= 0) & (inside < 11), roll(one[b], 32 * b - J), last)
            last = jnp.where((inside >= 11) & (inside < J), roll(one[b], 32 * b - 42), last)
        halves.append(swap_blocks(one) + swap_blocks(two) + [last])
    return [jnp.concatenate([halves[0][w], halves[1][w]], axis=1) for w in range(V)]


def kernel(
    n_dom,
    n_sub,
    levels_hbm,
    source_hbm,
    send_hbm,
    fault_flux_hbm,
    fault_faces_hbm,
    dofs_hbm,
    stiff_hbm,
    proj_hbm,
    star_hbm,
    minus_hbm,
    plus_hbm,
    out_ref,
    levels_ref,
    source_ref,
    send_ref,
    fault_flux_ref,
    fault_faces_ref,
    dofs_ref,
    stiff_ref,
    proj_ref,
    star_ref,
    minus_ref,
    plus_ref,
    block_ref,
    pt_ref,
    x_ref,
    row_ref,
    wd_ref,
    wv_ref,
    pw_ref,
    pt3_ref,
    ptw_ref,
    cs_ref,
    cm_ref,
    cc_ref,
    flux_ref,
    msg_ref,
    recv_ref,
    in_sem,
    send_sem,
    recv_sem,
    across_sem,
):
    dom = lax.axis_index("dom")
    sub = lax.axis_index("sub")
    peers = []
    for delta, turn in FARTHEST_FIRST:
        peers.append((delta, lax.rem(dom + delta + n_dom, n_dom), lax.rem(sub + turn, n_sub)))

    def strided(src, dst, count, at):
        return [
            pltpu.make_async_copy(
                src.at[:, w], dst.at[:, pl.ds(4 * w, count), :], in_sem.at[at]
            )
            for w in range(V)
        ]

    star_loads = strided(star_hbm, star_ref, 3, 8)
    minus_loads = strided(minus_hbm, minus_ref, 4, 9)
    plus_loads = strided(plus_hbm, plus_ref, 4, 10)
    loads = [
        pltpu.make_async_copy(src, dst, in_sem.at[i])
        for i, (src, dst) in enumerate(
            (
                (stiff_hbm, stiff_ref),
                (dofs_hbm, dofs_ref),
                (proj_hbm, proj_ref),
                (send_hbm, send_ref),
                (levels_hbm, levels_ref),
                (source_hbm, source_ref),
                (fault_flux_hbm, fault_flux_ref),
                (fault_faces_hbm, fault_faces_ref),
            )
        )
    ]
    for load in loads[0:1] + star_loads + loads[1:] + minus_loads + plus_loads:
        load.start()

    def wait_whole(src, at):
        pltpu.make_async_copy(src, src, in_sem.at[at]).wait()

    def wait(*which):
        for load in which:
            load.wait()

    odd = lax.rem(dom, 2)
    step = 2 * odd - 1
    partner = dom - step
    across = lax.rem(dom + step + n_dom, n_dom)
    behind = lax.rem(dom + 2 * step + n_dom, n_dom)
    subs = [lax.rem(sub + turn, n_sub) for turn in range(4)]
    barrier = pltpu.get_barrier_semaphore()

    def signal(to_dom, to_sub, which=barrier):
        pl.semaphore_signal(which, inc=1, device_id=(to_dom, to_sub), device_id_type=MESH)

    signal(behind, sub)
    for turn in (2, 1, 3):
        signal(dom, subs[turn])

    @pl.when(odd == 0)
    def _():
        for turn in (2, 1, 3):
            signal(behind, subs[turn])

    for turn in (2, 1, 3, 0):
        signal(partner, subs[turn])

    block_ref[...] = jnp.zeros(block_ref.shape, F32)
    pt_ref[...] = jnp.zeros(pt_ref.shape, F32)
    x_ref[...] = jnp.zeros(x_ref.shape, F32)
    row_ref[...] = jnp.zeros(row_ref.shape, F32)

    wait(loads[0])
    for d in range(3):
        block_ref[d, 0:M, 0:M] = stiff_ref[d]
        block_ref[d, 64 : 64 + M, 64 : 64 + M] = stiff_ref[d]
    for d in range(3):
        block = block_ref[d]
        wd_ref[:, 128 * d : 128 * d + 128] = rhs3(block.T)
        wv_ref[:, 128 * d : 128 * d + 128] = rhs3(block)

    wait(loads[2])
    for f in range(4):
        for half in range(2):
            at = 64 * f + 32 * half
            pt_ref[at : at + J, 64 * half : 64 * half + M] = proj_ref[:, f, :]
    pt = pt_ref[...]
    pw_ref[...] = rhs3(pt.T)

    wait(loads[3])
    row = rows((8, 256))
    lane = lanes((8, 256))
    wanted = jnp.full((8, 256), -1, jnp.int32)
    for s in range(4):
        wanted = jnp.where(row % 4 == s, send_ref[s], wanted)
    pick_send = ((lane % 64 == wanted) & (lane // 128 == row // 4)).astype(F32).astype(BF16)

    def spread(make_row, groups, part_width, fill, coef_ref):
        width = 128 * coef_ref.shape[3] // 128
        k = lax.broadcasted_iota(jnp.int32, (128, width), 0) % 64
        lane = lax.broadcasted_iota(jnp.int32, (128, width), 1)
        group = lane // (2 * part_width)
        half = (lane // part_width) % 2
        hit = (k // E == group) & ((k % E) // 8 == half) & (lane % part_width < fill)
        repeat = hit.astype(F32).astype(BF16)
        keep = (lanes() % 8 == rows()).astype(F32)
        for v in range(V):
            row = make_row(v)
            high = row.astype(BF16).astype(F32)
            row_ref[v, 0:V, 0 : groups * E] = high
            row_ref[v, 0:V, 64 : 64 + groups * E] = row - high
        for v in range(V):
            left = jnp.concatenate(
                [jnp.broadcast_to(row_ref[v, w : w + 1, :], (8, 128)) * keep for w in range(V)],
                axis=0,
            ).astype(BF16)
            coef_ref[v] = dot(left, repeat).reshape(V, 8, width)

    wait_whole(star_hbm, 8)
    spread(
        lambda v: jnp.concatenate([star_ref[v, pl.ds(d, V, stride=4), :] for d in range(3)], axis=1),
        3,
        64,
        M,
        cs_ref,
    )

    wait(loads[1])
    for v in range(V):
        x_ref[8 * v : 8 * v + 8, 0:M] = dofs_ref[v, 0:8, :]
        x_ref[8 * v : 8 * v + 8, 64 : 64 + M] = dofs_ref[v, 8:16, :]

    def contract(coef_ref, field, v):
        return (coef_ref[v] * field).sum(axis=0)

    def with_star(weights_ref, left):
        return star_sum(dot(left, weights_ref[...]))

    def star_sum(field):
        field = field.reshape(V, 8, 384)
        result = []
        for v in range(V):
            total = contract(cs_ref, field, v)
            result.append(total[:, 0:128] + total[:, 128:256] + total[:, 256:384])
        return jnp.concatenate(result, axis=0)

    def series(start, want_second, opening=None):
        current = start
        first = FIRST[0] * current
        second = SECOND[0] * current if want_second else None
        for k in range(1, ORDER):
            if k == 1 and opening is not None:
                current = star_sum(opening)
            else:
                current = with_star(wd_ref, lhs3(current))
            first = first + FIRST[k] * current
            if want_second:
                second = second + SECOND[k] * current
        return first, second

    dofs = x_ref[...]
    first_half, second_half = series(dofs, True)
    pl.semaphore_wait(barrier, 11 - 3 * odd)
    signal(partner, sub, across_sem)

    def make_message(turn, table):
        stacked = jnp.concatenate([stack2(table[0]), stack2(table[1])], axis=0)
        message = dot(pick_send, stacked)
        msg_ref[turn] = message
        recv_ref[turn, 4 + sub] = message

    def message_to(turn, slot, to_dom, to_sub, arrival):
        return pltpu.make_async_remote_copy(
            src_ref=msg_ref.at[turn],
            dst_ref=recv_ref.at[turn, slot],
            send_sem=send_sem.at[turn],
            recv_sem=arrival,
            device_id=(to_dom, to_sub),
            device_id_type=MESH,
        )

    def several(turn, count, arrival):
        some = recv_ref.at[turn, pl.ds(0, count)]
        return pltpu.make_async_remote_copy(
            src_ref=some,
            dst_ref=some,
            send_sem=send_sem.at[turn],
            recv_sem=arrival,
            device_id=(dom, subs[1]),
            device_id_type=MESH,
        )

    def start_first():
        @pl.when(odd == 1)
        def _():
            pl.semaphore_wait(across_sem, 1)
            for turn in (2, 1, 3, 0):
                message_to(0, sub, across, subs[turn], recv_sem.at[0]).start()

        for turn in (2, 1, 3):
            message_to(0, 4 + sub, dom, subs[turn], recv_sem.at[2]).start()
        for turn in (2, 1, 3, 0):
            message_to(0, 8 * odd + sub, partner, subs[turn], recv_sem.at[0]).start()

    def finish_first():
        several(0, 3, recv_sem.at[2]).wait_recv()

        @pl.when(odd == 0)
        def _():
            pl.semaphore_wait(across_sem, 1)
            pltpu.make_async_remote_copy(
                src_ref=recv_ref.at[0, pl.ds(4, 4)],
                dst_ref=recv_ref.at[0, pl.ds(8, 4)],
                send_sem=send_sem.at[0],
                recv_sem=recv_sem.at[0],
                device_id=(across, sub),
                device_id_type=MESH,
            ).start()

        several(0, 8, recv_sem.at[0]).wait_recv()

    def start_second():
        for delta, to_dom, to_sub in peers:
            message_to(1, 4 * (1 - delta) + sub, to_dom, to_sub, recv_sem.at[1]).start()

    def face_values(left):
        return dot(left[:, 0:256], pw_ref[0:256, :]) + dot(left[:, 256:384], pw_ref[256:384, :])

    def local_part(table):
        return dot(pick_local, jnp.concatenate([stack2(table[0]), stack2(table[1])], axis=1))

    def beside_faces(turn, near):
        arrived = stack2(recv_ref[turn].reshape(8 * SLOTS, 128))
        faces = from_table(
            near[:, 0:128] + dot(pick_remote[0:64], arrived),
            near[:, 128:256] + dot(pick_remote[64:128], arrived),
        )
        return jnp.concatenate(faces, axis=0).reshape(V, 8, 256)

    left = lhs3(first_half)
    faces = face_values(left)
    table = to_table(faces)
    make_message(0, table)
    start_first()

    pt3_ref[...] = rhs3(pt)
    wait(*loads[4:6])
    local_rows, remote_rows = [], []
    row = rows()
    lane = lanes()
    lane2 = lanes((8, 192)) % 96
    for f in range(4):
        for half in range(2):
            wanted = jnp.full((8, 128), -1, jnp.int32)
            for i in range(8):
                wanted = jnp.where(row == i, source_ref[f, 8 * half + i], wanted)
            local_rows.append((lane % 64 == wanted).astype(F32))
            far = wanted - 64
            code = jnp.where(far >= 0, (far // 4) * 8 + far % 4, -8)
            code = jnp.concatenate([code, code[:, 0:64]], axis=1)
            remote_rows.append((code, lane2))
    pick_local = jnp.concatenate(local_rows, axis=0).astype(BF16)
    pick_remote = jnp.concatenate(
        [(at == code + 4 * q).astype(F32) for q in range(2) for code, at in remote_rows], axis=0
    ).astype(BF16)

    fine = jnp.zeros((8, 128), jnp.int32)
    for e in range(E):
        here = (row == e % 8) & (lane // 64 == e // 8)
        fine = jnp.where(here & (levels_ref[e] == 0), 1, fine)
    fine = jnp.concatenate([fine] * V, axis=0) == 1

    wait_whole(minus_hbm, 9)
    spread(
        lambda v: jnp.concatenate([minus_ref[v, pl.ds(f, V, stride=4), :] for f in range(4)], axis=1),
        4,
        32,
        J,
        cm_ref,
    )
    wait_whole(plus_hbm, 10)
    wait(*loads[6:8])
    on_fault = jnp.concatenate([fault_faces_ref[f : f + 1, :] for f in range(4)], axis=1) == 1

    def coupling_row(v):
        plus = jnp.concatenate([plus_ref[v, pl.ds(f, V, stride=4), :] for f in range(4)], axis=1)
        w_at = rows((V, 4 * E))
        friction = jnp.zeros((V, 4 * E), F32)
        for w in range(V):
            friction = jnp.where(w_at == w, fault_flux_ref[v, w], friction)
        return jnp.where(jnp.broadcast_to(on_fault, (V, 4 * E)), friction, plus)

    spread(coupling_row, 4, 32, J, cc_ref)

    def own_side(left, faces):
        volume = with_star(wv_ref, left)
        field = faces.reshape(V, 8, 256)
        for v in range(V):
            flux_ref[8 * v : 8 * v + 8, :] = contract(cm_ref, field, v)
        return volume

    def fluxes(turn, near):
        field = beside_faces(turn, near)
        total = jnp.concatenate([contract(cc_ref, field, v) for v in range(V)], axis=0)
        hi, lo = split(total + flux_ref[...])
        return jnp.concatenate([hi, lo], axis=1), hi

    near = local_part(table)
    base = dofs + own_side(left, faces)
    base_slopes = dot(lhs3(base), wd_ref[...])
    ptw_ref[...] = rhs3(dot(lhs3(pt), wd_ref[...]))
    finish_first()
    both, hi = fluxes(0, near)
    opening = base_slopes - dot(both, ptw_ref[0:512, :]) - dot(hi, ptw_ref[512:768, :])
    moved = base - dot(both, pt3_ref[0:512, :]) - dot(hi, pt3_ref[512:768, :])

    again, _ = series(moved, False, opening)
    carried = jnp.where(fine, again, second_half)
    left = lhs3(carried)
    faces = face_values(left)
    table = to_table(faces)
    make_message(1, table)
    start_second()
    near = local_part(table)
    base = moved + own_side(left, faces)
    for turn in range(2):
        several(turn, len(peers), recv_sem.at[turn]).wait_send()
    several(1, len(peers), recv_sem.at[1]).wait_recv()
    both, hi = fluxes(1, near)
    after = base - dot(both, pt3_ref[0:512, :]) - dot(hi, pt3_ref[512:768, :])
    for v in range(V):
        out_ref[v, 0:8, :] = after[8 * v : 8 * v + 8, 0:M]
        out_ref[v, 8:16, :] = after[8 * v : 8 * v + 8, 64 : 64 + M]


def per_device(
    n_dom,
    n_sub,
    dofs,
    stiffness,
    projection,
    star,
    flux_minus,
    flux_plus,
    fault_flux,
    fault_faces,
    levels,
    face_source,
    send_source,
):
    vmem = pl.BlockSpec(memory_space=pltpu.VMEM)
    hbm = pl.BlockSpec(memory_space=pltpu.HBM)
    result = pl.pallas_call(
        functools.partial(kernel, n_dom, n_sub),
        out_shape=pltpu.VMEM((V, E, M), F32),
        in_specs=[hbm] * 11,
        out_specs=vmem,
        scratch_shapes=[
            pltpu.SMEM((E,), jnp.int32),
            pltpu.SMEM((4, E), jnp.int32),
            pltpu.SMEM((4,), jnp.int32),
            pltpu.SMEM((V, V), F32),
            pltpu.VMEM((4, E), jnp.int32),
            pltpu.VMEM((V, E, M), F32),
            pltpu.VMEM((3, M, M), F32),
            pltpu.VMEM((J, 4, M), F32),
            pltpu.VMEM((V, 4 * V, E), F32),
            pltpu.VMEM((V, 4 * V, E), F32),
            pltpu.VMEM((V, 4 * V, E), F32),
            pltpu.VMEM((3, 128, 128), F32),
            pltpu.VMEM((256, 128), F32),
            pltpu.VMEM((72, 128), F32),
            pltpu.VMEM((V, 16, 128), F32),
            pltpu.VMEM((384, 384), BF16),
            pltpu.VMEM((384, 384), BF16),
            pltpu.VMEM((384, 256), BF16),
            pltpu.VMEM((768, 128), BF16),
            pltpu.VMEM((768, 384), BF16),
            pltpu.VMEM((V, V, 8, 384), F32),
            pltpu.VMEM((V, V, 8, 256), F32),
            pltpu.VMEM((V, V, 8, 256), F32),
            pltpu.VMEM((72, 256), F32),
            pltpu.VMEM((2, 8, 128), F32),
            pltpu.VMEM((2, SLOTS, 8, 128), F32),
            pltpu.SemaphoreType.DMA((11,)),
            pltpu.SemaphoreType.DMA((2,)),
            pltpu.SemaphoreType.DMA((3,)),
            pltpu.SemaphoreType.REGULAR,
        ],
        compiler_params=pltpu.CompilerParams(
            collective_id=0, has_side_effects=True, vmem_limit_bytes=VMEM_LIMIT
        ),
    )(
        *(
            pltpu.with_memory_space_constraint(x, pltpu.HBM)
            for x in (
        levels,
        face_source,
        send_source,
        fault_flux,
        fault_faces,
        jnp.transpose(dofs, (0, 2, 1)),
        stiffness,
        jnp.transpose(projection, (1, 0, 2)),
        jnp.transpose(star, (1, 2, 0, 3)),
        jnp.transpose(flux_minus, (1, 2, 0, 3)),
        jnp.transpose(flux_plus, (1, 2, 0, 3)),
                )
        )
    )
    return jnp.transpose(result, (0, 2, 1))


def solution(mesh):
    return jax.shard_map(
        functools.partial(per_device, mesh.shape["dom"], mesh.shape["sub"]),
        mesh=mesh,
        in_specs=(
            P(None, None, ("dom", "sub")),
            P(),
            P(),
            P(None, None, None, ("dom", "sub")),
            P(None, None, None, ("dom", "sub")),
            P(None, None, None, ("dom", "sub")),
            P(),
            P(None, ("dom", "sub")),
            P(("dom", "sub")),
            P(None, ("dom", "sub")),
            P(("dom", "sub")),
        ),
        out_specs=P(None, None, ("dom", "sub")),
        check_vma=False,
    )
```
